256 devices in a mesh: dp: 8 (over x, core), expert: 32 (over y, z).
Axes of the slice: x: 4, y: 4, z: 8, core: 2. Of those that a mesh axis runs over, the one named last changes fastest.
Arguments:
- queries: bfloat16 [2, 8, 32, 2048], P(None, 'dp', 'expert'), may hold values from -5 to 5
- cache_keys: bfloat16 [8, 32, 512, 512], P('dp', 'expert'), may hold values from -5 to 5
- cache_values: bfloat16 [8, 32, 512, 512], P('dp', 'expert'), may hold values from -6 to 6
- new_keys: bfloat16 [2, 8, 32, 512], P(None, 'dp', 'expert'), may hold values from -9 to 9
- new_values: bfloat16 [2, 8, 32, 512], P(None, 'dp', 'expert'), may hold values from -6 to 6
- cache_len: int32 [8, 32], P('dp', 'expert'), may hold values from 256 to 510, as said below
- o_proj: bfloat16 [2048, 4096], P(None, 'expert'), may hold values from -0.125 to 0.125
- residual_in: bfloat16 [2, 8, 32, 4096], P(None, 'dp', None, 'expert'), may hold values from -36 to 36
- norm_gain: float32 [4096], P('expert'), may hold values from 0.1 to 1.9
- router: float32 [4096, 8], P('expert'), may hold values from -0.09375 to 0.09375
- expert_gate: bfloat16 [32, 4096, 3584], P('expert', None, 'dp'), may hold values from -0.09375 to 0.09375
- expert_up: bfloat16 [32, 4096, 3584], P('expert', None, 'dp'), may hold values from -0.09375 to 0.09375
- expert_down: bfloat16 [32, 3584, 4096], P('expert', 'dp'), may hold values from -0.046875 to 0.046875
- routes: int32 [2, 8, 32, 2], replicated, may hold values from 0 to 7, all different within a row; in each aligned block of 32 rows (0 to 31, 32 to 63, ..., all dimensions but the last counted through in order) at most 16 rows name the same one
- answers: int32 [2, 8, 32], P(None, 'dp', 'expert'), may hold values from 0 to 127
- stop_mask: int32 [2, 8], P(None, 'dp'), may hold values 0 or 1
Outputs:
- residual_out: bfloat16 [2, 8, 32, 4096], P(None, 'dp', None, 'expert')
- vote_share: float32 [2, 8, 128], P(None, 'dp')
The draws below stay inside these ranges and needn't reach their ends.
Inputs may be any that keep to these rules, and one draw needn't show every extreme that they name: `cache_len`: some sequence uses exactly 510 cached positions. `routes`: each token names 2 different experts; in each step, the tokens of the 1 prompts of one index of dp (all their samples together) name one expert at most 16 times.
All inputs are finite; a program needn't handle non-finite values. No bound on the sum of `stop_mask` on one device may be relied on, other than what follows from the above.
Results may differ from the reference program's by a relative error of at most 0.0055.
Values may be sent and summed in bfloat16 or wider, within the bound.
A program may use at most 64 MiB of HBM per device.

```python
import math
import jax
import jax.numpy as jnp
import numpy as np
from jax import lax

D = 4096
E = 8
TOP = 2
HD = 128
QH = 16
KVH = 4
FFW = 14336
STEPS = 2
ANSWERS = 128
CACHE = 512
PROMPT_DEV = 1
PROMPTS = 8
SAMPLES = 32
SPLIT = 4
CAP = 16


def draw_queries(key, part):
    noise_key = jax.random.fold_in(key, 3)
    full_shape = (STEPS, PROMPTS, SAMPLES, QH * HD)
    return jnp.clip(2.0 * jax.random.normal(noise_key, full_shape, jnp.float32), -5.0, 5.0).astype(jnp.bfloat16)


def draw_cache_keys(key, part):
    noise_key = jax.random.fold_in(key, 5)
    full_shape = (PROMPTS, SAMPLES, CACHE, KVH * HD)
    return jnp.clip(jax.random.normal(noise_key, full_shape, jnp.float32), -4.0, 4.0).astype(jnp.bfloat16)


def draw_residual_in(key, part):
    noise_key = jax.random.fold_in(jax.random.fold_in(key, 11), 0)
    full_shape = (STEPS, PROMPTS, SAMPLES, D)
    values = jnp.clip(jax.random.normal(noise_key, full_shape, jnp.float32), -4.0, 4.0)
    return values.astype(jnp.bfloat16)


def draw_cache_len(key, part):
    lengths = jax.random.randint(jax.random.fold_in(key, 13), (PROMPTS, SAMPLES), CACHE // 2, CACHE - STEPS + 1, dtype=jnp.int32)
    return lengths.at[0, 0].set(CACHE - STEPS)


def touch_ends(values, rng, least, top_value):
    spot = [jax.random.randint(jax.random.fold_in(rng, axis), (), 0, length) for axis, length in enumerate(values.shape)]
    widest = values.shape.index(max(values.shape))
    beside = spot[:widest] + [(spot[widest] + 1) % values.shape[widest]] + spot[widest + 1:]
    return values.at[tuple(spot)].set(least).at[tuple(beside)].set(top_value)


def block_levels(stream_key, shape, pieces, smallest, high):
    loudness = 1.0
    for position, parts in pieces:
        draws = jax.random.uniform(jax.random.fold_in(jax.random.fold_in(stream_key, 6), position), (parts,), jnp.float32, smallest / len(pieces), high / len(pieces))
        loudness = loudness * jnp.repeat(jnp.exp(draws), shape[position] // parts).reshape((-1,) + (1,) * (len(shape) - 1 - position))
    return loudness


def rank_table(count, skew):
    loads = [(1 << 20) // math.isqrt(rank ** skew) + 1 for rank in range(1, count + 1)]
    width = 1 + sum(loads) // (1 << 30)
    return np.cumsum(np.array([max(1, weight // width) for weight in loads]))


def skewed_ids(stream_key, dims, number_of, lean):
    listing = rank_table(number_of, lean)
    lot = jax.random.randint(jax.random.fold_in(stream_key, 1), dims, 0, int(listing[number_of - 1]))
    rank = jnp.searchsorted(jnp.asarray(listing, jnp.int32), lot, side="right")
    return jax.random.permutation(jax.random.fold_in(stream_key, 2), number_of)[rank].astype(jnp.int32)


def assign_block(stream_key, own, number, rows, count, top, bound, lean):
    order = jax.random.permutation(stream_key, count)
    heavy_load, ordinary = portions_of(count, rows * top, bound, lean, True), portions_of(count, rows * top, bound, lean, False)
    places = jnp.arange(count)

    def named(tallies, rotation):
        used = int((tallies > 0).sum())
        fixed = max(1, used // 4)
        moved = fixed + (places - fixed + rotation * (used - fixed)) % max(1, count - fixed)
        return jnp.zeros((count,), jnp.int32).at[order[jnp.where(places < fixed, places, moved)]].set(jnp.asarray(tallies, jnp.int32))

    tallies = jnp.where(number % 4 == 0, named(heavy_load, number // 4), named(ordinary, number - number // 4 - 1))
    mixed = jax.random.permutation(jax.random.fold_in(own, 3), count)
    giver, sink = mixed[0:count // 2 * 2:2], mixed[1:count // 2 * 2:2]
    slack = jnp.minimum(tallies[giver] - 1, bound - tallies[sink]) // 2
    slack = jnp.where((giver == order[0]) | (sink == order[0]) | (tallies[sink] == 0), 0, jnp.maximum(slack, 0))
    moved = jax.random.randint(jax.random.fold_in(own, 4), (count // 2,), 0, 1 << 20) % (slack + 1)
    tallies = tallies.at[giver].add(-moved).at[sink].add(moved)
    labels = jnp.searchsorted(jnp.cumsum(tallies), jnp.arange(rows * top), side="right").astype(jnp.int32)
    table = labels.reshape(top, rows).T
    table = table[jax.random.permutation(jax.random.fold_in(own, 1), rows)]
    rotation = jax.random.randint(jax.random.fold_in(own, 2), (rows, 1), 0, top)
    return jnp.take_along_axis(table, (jnp.arange(top)[None, :] + rotation) % top, axis=1)


def portions_of(amount, total, reach, skew, full):
    portions = [(1 << 20) // math.isqrt(grade ** skew) + 1 for grade in range(1, amount + 1)]
    largest = reach if full else min(reach, max(-(-total // amount), total * portions[0] // sum(portions)))
    least = 1 if total - largest >= amount - 1 else 0
    given, rest = [largest] + [least] * (amount - 1), total - largest - least * (amount - 1)
    while rest > 0:
        movable = [i for i in range(1, amount) if given[i] < largest] or [i for i in range(1, amount) if given[i] < reach]
        mass, remaining = sum([portions[i] for i in movable]), rest
        for i in movable:
            extra = min(reach - given[i], max(1, remaining * portions[i] // mass), rest)
            given[i] = given[i] + extra
            rest = rest - extra
    return np.array(given)


def noise(own_key, shape, deviation, most, cuts=(), kind=jnp.bfloat16):
    factor_of = block_levels(own_key, shape, cuts, -0.22, 0.18) if cuts else 1.0
    entries = jax.random.normal(own_key, shape, jnp.float32) * deviation * factor_of
    return jnp.minimum(jnp.maximum(entries, -most), most).astype(kind)


def setup_inputs(seed: int = 0) -> dict:
    arg_keys = jax.random.split(jax.random.key(seed), 17)
    queries = draw_queries(jax.random.fold_in(arg_keys[16], 71), 0)
    cache_keys = draw_cache_keys(jax.random.fold_in(arg_keys[16], 71), 0)
    cache_values = noise(arg_keys[2], (PROMPTS, SAMPLES, CACHE, KVH * HD), 1.0, 6.0, ((0, 8), (1, 32)))
    new_keys = noise(arg_keys[3], (STEPS, PROMPTS, SAMPLES, KVH * HD), 1.5, 9.0, ((1, 8), (2, 32)))
    new_values = noise(arg_keys[4], (STEPS, PROMPTS, SAMPLES, KVH * HD), 1.0, 6.0, ((1, 8), (2, 32)))
    cache_len = draw_cache_len(jax.random.fold_in(arg_keys[16], 71), 0)
    o_proj = noise(arg_keys[6], (QH * HD, D), (QH * HD) ** -0.5, 0.125, ((1, 32),))
    residual_in = draw_residual_in(jax.random.fold_in(arg_keys[16], 71), 0)
    norm_gain = jnp.clip(1.0 + 0.18 * jax.random.normal(arg_keys[8], (D,), jnp.float32), 0.1, 1.9)
    router = noise(arg_keys[9], (D, E), D ** -0.5, 0.09375, ((0, 32),), jnp.float32)
    expert_gate = noise(arg_keys[10], (E * SPLIT, D, FFW // SPLIT), D ** -0.5, 0.09375, ((0, 32), (2, 8)))
    expert_up = noise(arg_keys[11], (E * SPLIT, D, FFW // SPLIT), D ** -0.5, 0.09375, ((0, 32), (2, 8)))
    expert_down = noise(arg_keys[12], (E * SPLIT, FFW // SPLIT, D), FFW ** -0.5, 0.046875, ((0, 32), (1, 8)))
    routes_keys = jax.random.split(jax.random.fold_in(arg_keys[13], 1), STEPS * PROMPTS * SAMPLES // (PROMPT_DEV * SAMPLES))
    routes_turns = jax.random.permutation(jax.random.fold_in(arg_keys[13], 3), STEPS * PROMPTS * SAMPLES // (PROMPT_DEV * SAMPLES))
    routes = jax.vmap(lambda own, number: assign_block(jax.random.fold_in(arg_keys[13], 2), own, number, PROMPT_DEV * SAMPLES, E, TOP, CAP, 1))(routes_keys, routes_turns).reshape((STEPS, PROMPTS, SAMPLES, TOP))
    answers = touch_ends(skewed_ids(arg_keys[14], (STEPS, PROMPTS, SAMPLES), ANSWERS, 2), jax.random.fold_in(arg_keys[14], 3), 0, ANSWERS - 1).astype(jnp.int32)
    stop_mask = touch_ends((jax.random.randint(arg_keys[15], (STEPS, PROMPTS), 0, 4) < 1).astype(jnp.int32), jax.random.fold_in(arg_keys[15], 1), 0, 1)
    return {"queries": queries, "cache_keys": cache_keys, "cache_values": cache_values, "new_keys": new_keys, "new_values": new_values, "cache_len": cache_len, "o_proj": o_proj, "residual_in": residual_in, "norm_gain": norm_gain, "router": router, "expert_gate": expert_gate, "expert_up": expert_up, "expert_down": expert_down, "routes": routes, "answers": answers, "stop_mask": stop_mask}


EPSILON = 1e-05

def attend(query, keys, values, fresh_keys, fresh_values, lengths):
    step_count = query.shape[0]
    row_count = query.shape[1]
    cache_size = keys.shape[1]
    group_size = QH // KVH
    score_scale = HD ** (-0.5)
    queried = query.astype(jnp.float32).reshape(step_count, row_count, KVH, group_size, HD)
    old_keys = keys.astype(jnp.float32).reshape(row_count, cache_size, KVH, HD)
    old_values = values.astype(jnp.float32).reshape(row_count, cache_size, KVH, HD)
    young_keys = fresh_keys.astype(jnp.float32).reshape(step_count, row_count, KVH, HD)
    young_values = fresh_values.astype(jnp.float32).reshape(step_count, row_count, KVH, HD)
    old_scores = jnp.einsum('trkgd,rckd->rkgtc', queried, old_keys) * score_scale
    new_scores = jnp.einsum('trkgd,urkd->rkgtu', queried, young_keys) * score_scale
    old_valid = jnp.arange(cache_size, dtype=jnp.int32)[None, :] < lengths[:, None]
    old_scores = jnp.where(old_valid[:, None, None, None, :], old_scores, -jnp.inf)
    new_valid = jnp.arange(step_count)[None, :] <= jnp.arange(step_count)[:, None]
    new_scores = jnp.where(new_valid, new_scores, -jnp.inf)
    highest = jnp.maximum(lax.optimization_barrier(jnp.max(old_scores, -1)), lax.optimization_barrier(jnp.max(new_scores, -1)))[..., None]
    old_exp = jnp.exp(old_scores - highest)
    new_exp = jnp.exp(new_scores - highest)
    denominator = lax.optimization_barrier(jnp.sum(old_exp, -1, keepdims=True)) + lax.optimization_barrier(jnp.sum(new_exp, -1, keepdims=True))
    old_weights = (old_exp / denominator).astype(jnp.bfloat16)
    new_weights = (new_exp / denominator).astype(jnp.bfloat16)
    combined = jnp.einsum('rkgtc,rckd->trkgd', old_weights.astype(jnp.float32), old_values)
    combined = combined + jnp.einsum('rkgtu,urkd->trkgd', new_weights.astype(jnp.float32), young_values)
    return combined.reshape(step_count, row_count, QH * HD).astype(jnp.bfloat16)

def per_prompt(operands):
    query, keys, values, fresh_keys, fresh_values, lengths = operands
    return attend(query, keys, values, fresh_keys, fresh_values, lengths)

def expert_pass(operands):
    tokens, w_gate, w_up, w_down = operands
    gate_part = jnp.dot(tokens, w_gate, preferred_element_type=jnp.float32)
    up_part = jnp.dot(tokens, w_up, preferred_element_type=jnp.float32)
    hidden = (jax.nn.silu(gate_part) * up_part).astype(jnp.bfloat16)
    return jnp.dot(hidden, w_down, preferred_element_type=jnp.float32)

def reference(queries, cache_keys, cache_values, new_keys, new_values, cache_len, o_proj, residual_in, norm_gain, router, expert_gate, expert_up, expert_down, routes, answers, stop_mask):
    attended = lax.map(per_prompt, (jnp.moveaxis(queries, 1, 0), cache_keys, cache_values, jnp.moveaxis(new_keys, 1, 0), jnp.moveaxis(new_values, 1, 0), cache_len))
    attended = jnp.moveaxis(attended, 0, 1)
    row_total = STEPS * PROMPTS * SAMPLES
    attn_proj = jnp.dot(attended.reshape(row_total, QH * HD), o_proj, preferred_element_type=jnp.float32)
    mixed_rows = residual_in.reshape(row_total, D).astype(jnp.float32) + attn_proj
    inv_rms = lax.rsqrt(lax.optimization_barrier(jnp.mean(mixed_rows * mixed_rows, -1, keepdims=True)) + EPSILON)
    normed_f = mixed_rows * inv_rms * norm_gain
    normed = normed_f.astype(jnp.bfloat16)
    logits = jnp.dot(normed_f, router, precision=lax.Precision.HIGHEST)
    picks = routes.reshape(row_total, TOP)
    chosen = jnp.take_along_axis(logits, picks, axis=1)
    gate_weights = jax.nn.sigmoid(chosen - chosen[:, ::-1])
    block_rows = PROMPT_DEV * SAMPLES
    block_count = row_total // block_rows
    expert_hot = (picks[:, :, None] == jnp.arange(E, dtype=jnp.int32)).astype(jnp.int32)
    flat_hot = expert_hot.reshape(block_count, block_rows * TOP, E)
    earlier = jnp.cumsum(flat_hot, axis=1) - flat_hot
    place = lax.optimization_barrier(jnp.sum(earlier * flat_hot, -1)).reshape(row_total, TOP)
    block_of = (jnp.arange(row_total, dtype=jnp.int32) // block_rows)[:, None]
    slot_ids = (picks * block_count + block_of) * CAP + place
    slot_total = E * block_count * CAP
    owners = jnp.zeros((slot_total,), jnp.int32).at[slot_ids.reshape(-1)].set(jnp.arange(row_total * TOP, dtype=jnp.int32) // TOP + 1)
    padded = jnp.concatenate([jnp.zeros((1, D), jnp.bfloat16), normed], 0)
    slot_rows = padded[owners].reshape(E, block_count * CAP, D)
    full_gate = expert_gate.reshape(E, SPLIT, D, FFW // SPLIT).transpose(0, 2, 1, 3).reshape(E, D, FFW)
    full_up = expert_up.reshape(E, SPLIT, D, FFW // SPLIT).transpose(0, 2, 1, 3).reshape(E, D, FFW)
    full_down = expert_down.reshape(E, FFW, D)
    expert_out = lax.map(expert_pass, (slot_rows, full_gate, full_up, full_down)).reshape(slot_total, D)
    picked = expert_out[slot_ids.reshape(-1)].reshape(row_total, TOP, D)
    moe = lax.optimization_barrier(jnp.sum(gate_weights[:, :, None] * picked, 1))
    active = (1 - stop_mask).astype(jnp.float32)
    active_rows = jnp.broadcast_to(active[:, :, None], (STEPS, PROMPTS, SAMPLES)).reshape(row_total, 1)
    updated = residual_in.reshape(row_total, D).astype(jnp.float32) + active_rows * (attn_proj + moe)
    residual_out = updated.reshape(STEPS, PROMPTS, SAMPLES, D).astype(jnp.bfloat16)
    hits = lax.optimization_barrier(jnp.sum((answers[..., None] == jnp.arange(ANSWERS, dtype=jnp.int32)).astype(jnp.float32), 2))
    votes = active[:, :, None] * hits
    tally = jnp.cumsum(votes, 0)
    vote_share = tally / jnp.maximum(lax.optimization_barrier(jnp.sum(tally, -1, keepdims=True)), 1.0)
    return (residual_out, vote_share)
```

```python
import jax
import jax.numpy as jnp
from jax import lax
from jax.experimental import pallas as pl
from jax.experimental.pallas import tpu as pltpu
from jax.sharding import PartitionSpec as P

D = 4096
E = 8
HD = 128
QH = 16
KVH = 4
STEPS = 2
ANSWERS = 128
EPSILON = 1e-05

ROWS = 64
PEERS = 32
LOCAL = 448
CHUNK = 1024
HALF = 512
SLOTS = 32
ORDER = (0, 1, 3, 2)

MESH = pl.DeviceIdType.MESH
F32 = jnp.float32
BF16 = jnp.bfloat16
NT = (((1,), (1,)), ((), ()))
NN = (((1,), (0,)), ((), ()))
NEG = -1e30


def dot(a, b, dims, precision=None):
    return lax.dot_general(a, b, dims, precision=precision, preferred_element_type=F32)


def iota(shape, dim):
    return lax.broadcasted_iota(jnp.int32, shape, dim)


def remote(src, dst, send_sem, recv_sem, device):
    return pltpu.make_async_remote_copy(
        src_ref=src,
        dst_ref=dst,
        send_sem=send_sem,
        recv_sem=recv_sem,
        device_id=device,
        device_id_type=MESH,
    )


def drain(ref, sem):
    pltpu.make_async_copy(ref, ref, sem).wait()


def layer(
    q_ref, nk_ref, nv_ref, len_ref, res_ref, gain_ref, router_ref, routes_ref, ans_ref, stop_ref,
    kc_ref, vc_ref, wo_hbm, wg_hbm, wu_hbm, wd_hbm,
    out_ref, share_ref,
    keys, values, wo, wg, wu, wd,
    qs, nks, nvs, att, attf, attm, stats, packed, disp, tok, gacc, uacc, hid,
    part, mate, zsum, hop_l, hop_r, fin, back, ret,
    load_sem, att_s, att_r, st_s, st_r, dp_s, dp_r,
    x_s, xl_r, xr_r, hl_r, hr_r, mt_r, y_s, my_r, yl_r, yr_r, fin_r, bk_s, bk_r,
):
    dp = lax.axis_index("dp")
    me = lax.axis_index("expert")
    x, c = lax.div(dp, 2), lax.rem(dp, 2)
    y, z = lax.div(me, 8), lax.rem(me, 8)
    xr, xl, xd = lax.rem(x + 1, 4), lax.rem(x + 3, 4), lax.rem(x + 2, 4)
    right, left, other = {"dp": xr * 2 + c}, {"dp": xl * 2 + c}, {"dp": x * 2 + 1 - c}
    expert = lax.div(me, 4)

    loads = [
        pltpu.make_async_copy(src, dst, load_sem.at[i])
        for i, (src, dst) in enumerate(
            (
                (kc_ref, keys),
                (vc_ref, values),
                (wo_hbm, wo),
                (wg_hbm, wg),
                (wu_hbm, wu),
                (wd_hbm, wd),
            )
        )
    ]
    for load in loads:
        load.start()

    barrier = pltpu.get_barrier_semaphore()

    def greet(i, carry):
        pl.semaphore_signal(
            barrier, inc=1, device_id={"expert": lax.rem(me + i, PEERS)}, device_id_type=MESH
        )
        return carry

    lax.fori_loop(1, PEERS, greet, 0)
    for neighbour in (right, left, other):
        pl.semaphore_signal(barrier, inc=1, device_id=neighbour, device_id_type=MESH)

    qf = q_ref[...].astype(F32)
    nkf = nk_ref[...].astype(F32)
    nvf = nv_ref[...].astype(F32)
    for kv in range(KVH):
        lanes = slice(kv * HD, (kv + 1) * HD)
        for t in range(STEPS):
            for g in range(4):
                h = kv * 4 + g
                r = kv * 8 + t * 4 + g
                qs[r : r + 1, :] = qf[t : t + 1, h * HD : (h + 1) * HD]
        for u in range(STEPS):
            nks[u, kv * 8 : kv * 8 + 8, :] = jnp.broadcast_to(nkf[u : u + 1, lanes], (8, HD))
            nvs[u, kv * 8 : kv * 8 + 8, :] = jnp.broadcast_to(nvf[u : u + 1, lanes], (8, HD))
    scale = HD ** (-0.5)
    qa = qs[...]
    qb = qa.astype(BF16)
    row = iota((32, 1), 0)
    second = lax.rem(lax.div(row, 4), 2) == 1
    fresh0 = jnp.sum(qa * nks[0], axis=1, keepdims=True) * scale
    fresh1 = jnp.sum(qa * nks[1], axis=1, keepdims=True) * scale
    fresh1 = jnp.where(second, fresh1, NEG)
    loads[0].wait()
    scores = jnp.concatenate(
        [
            dot(qb[kv * 8 : kv * 8 + 8], keys[:, kv * HD : (kv + 1) * HD], NT)
            for kv in range(KVH)
        ],
        axis=0,
    )
    scores = scores * scale
    scores = jnp.where(iota((32, 512), 1) < len_ref[0, 0], scores, NEG)
    top = jnp.maximum(jnp.maximum(jnp.max(scores, axis=1, keepdims=True), fresh0), fresh1)
    old = jnp.exp(scores - top)
    new0 = jnp.exp(fresh0 - top)
    new1 = jnp.exp(fresh1 - top)
    total = jnp.sum(old, axis=1, keepdims=True) + new0 + new1
    old = (old / total).astype(BF16)
    new0 = (new0 / total).astype(BF16).astype(F32)
    new1 = (new1 / total).astype(BF16).astype(F32)
    loads[1].wait()
    mixed_values = jnp.concatenate(
        [
            dot(old[kv * 8 : kv * 8 + 8], values[:, kv * HD : (kv + 1) * HD], NN)
            for kv in range(KVH)
        ],
        axis=0,
    )
    mixed_values = mixed_values + new0 * nvs[0] + new1 * nvs[1]
    att[me] = mixed_values.astype(BF16)

    pl.semaphore_wait(barrier, PEERS + 2)

    def send_att(i, carry):
        peer = lax.rem(me + i, PEERS)
        remote(att.at[me], att.at[me], att_s, att_r, {"expert": peer}).start()
        return carry

    lax.fori_loop(1, PEERS, send_att, 0)

    picks = jnp.concatenate([routes_ref[0, dp], routes_ref[1, dp]], axis=1)
    pick0, pick1 = picks[0:1, :], picks[1:2, :]
    names = iota((E, ROWS), 0)
    hot0, hot1 = (names == pick0).astype(F32), (names == pick1).astype(F32)
    a, b = iota((ROWS, ROWS), 0), iota((ROWS, ROWS), 1)
    before = ((a < b) & (lax.div(a, 32) == lax.div(b, 32))).astype(F32)
    earlier = dot((hot0 + hot1).astype(BF16), before.astype(BF16), NN)
    step_base = lax.div(iota((1, ROWS), 1), 32) * 16
    place0 = jnp.sum(earlier * hot0, axis=0, keepdims=True).astype(jnp.int32)
    place1 = jnp.sum(earlier * hot1, axis=0, keepdims=True).astype(jnp.int32)
    slot0 = pick0 * SLOTS + step_base + place0
    slot1 = pick1 * SLOTS + step_base + place1
    slots = iota((E * SLOTS, ROWS), 0)
    table = ((slots == slot0) | (slots == slot1)).astype(F32).astype(BF16)
    mine = iota((SLOTS, ROWS), 0) + expert * SLOTS
    own_table = ((mine == slot0) | (mine == slot1)).astype(F32)
    eye = a == b
    col0 = jnp.sum(jnp.where(eye, jnp.broadcast_to(slot0, (ROWS, ROWS)), 0), axis=1, keepdims=True)
    col1 = jnp.sum(jnp.where(eye, jnp.broadcast_to(slot1, (ROWS, ROWS)), 0), axis=1, keepdims=True)
    sign = hot0 - hot1
    sign_rows = dot(eye.astype(F32).astype(BF16), sign.astype(BF16), NT)

    hits = jnp.concatenate(
        [
            (iota((1, ANSWERS), 1) == ans_ref[0, t]).astype(F32)
            * (1 - stop_ref[0, t]).astype(F32)
            for t in range(STEPS)
        ],
        axis=0,
    )

    loads[2].wait()
    drain(att.at[0 : PEERS - 1], att_r)
    attf[...] = att[...].astype(F32).reshape(PEERS * 32, HD)
    for t in range(STEPS):
        for h in range(QH):
            r = (h // 4) * 8 + t * 4 + h % 4
            attm[t * 32 : (t + 1) * 32, h * HD : (h + 1) * HD] = attf[
                pl.ds(r, 32, stride=32), :
            ].astype(BF16)
    attn_proj = dot(attm[...], wo[...], NN)
    residual = res_ref[...].reshape(ROWS, HD).astype(F32)
    mixed = residual + attn_proj
    scaled = mixed * gain_ref[...].reshape(1, HD)
    squares = jnp.sum(mixed * mixed, axis=1, keepdims=True)
    logits = dot(scaled, router_ref[...], NT, lax.Precision.HIGHEST)
    apart = jnp.sum(logits * sign_rows, axis=1, keepdims=True)
    lane, line = iota((ROWS, 128), 1), iota((ROWS, 128), 0)
    line_up = jnp.where(lane == line, squares, jnp.where(lane == line + ROWS, apart, 0.0))
    stats[me, 0:1, :] = jnp.sum(line_up, axis=0, keepdims=True)
    stats[me, 1:3, :] = hits
    stats[me, 3:4, :] = jnp.zeros((1, 128), F32)

    def send_stats(i, carry):
        peer = lax.rem(me + i, PEERS)
        remote(stats.at[me], stats.at[me], st_s, st_r, {"expert": peer}).start()
        return carry

    lax.fori_loop(1, PEERS, send_stats, 0)

    packed[...] = dot(table, scaled.astype(BF16), NN).astype(BF16).reshape(E, SLOTS, HD)

    for dy in range(4):
        yd = lax.rem(y + dy, 4)

        def send_tokens(i, carry, dy=dy, yd=yd):
            peer = yd * 8 + lax.rem(z + i, 8)
            remote(
                packed.at[lax.div(peer, 4)],
                disp.at[me],
                dp_s,
                dp_r.at[(4 - dy) % 4],
                {"expert": peer},
            ).start()
            return carry

        lax.fori_loop(1 if dy == 0 else 0, 8, send_tokens, 0)
    disp[me] = packed[expert]

    cols = iota((ROWS, PEERS * SLOTS), 1)
    ids = lax.div(cols, 128) * SLOTS + lax.rem(cols, SLOTS)
    comb0 = (ids == col0).astype(F32).astype(BF16)
    comb1 = (ids == col1).astype(F32).astype(BF16)

    drain(stats.at[0 : PEERS - 1], st_r)
    sums = jnp.sum(stats[...], axis=0)
    squares_row, apart_row = sums[0:1, 0:ROWS], sums[0:1, ROWS:128]
    inv_row = lax.rsqrt(squares_row * (1.0 / D) + EPSILON)
    own_inv = jnp.sum(own_table * inv_row, axis=1, keepdims=True)
    gap_row = apart_row * inv_row
    gap = jnp.sum(jnp.where(eye, jnp.broadcast_to(gap_row, (ROWS, ROWS)), 0.0), axis=1, keepdims=True)
    tally0 = sums[1:2, :]
    tally1 = tally0 + sums[2:3, :]
    share_ref[0] = tally0 / jnp.maximum(jnp.sum(tally0, axis=1, keepdims=True), 1.0)
    share_ref[1] = tally1 / jnp.maximum(jnp.sum(tally1, axis=1, keepdims=True), 1.0)

    def block(xp, cp):
        return pl.ds(pl.multiple_of((cp * 4 + xp) * SLOTS, SLOTS), SLOTS)

    low, high = pl.ds(0, HALF), pl.ds(HALF, HALF)

    def spread_own(i):
        off = ORDER[i]
        qy = lax.rem(y + off, 4)
        drain(disp.at[0 : 7 if off == 0 else 8], dp_r.at[off])
        for k in range(8):
            rows = disp[qy * 8 + k].astype(F32) * own_inv
            tok[i, block(x, c), k * HD : (k + 1) * HD] = rows.astype(BF16)
        src = tok.at[i, block(x, c)]
        remote(src, src, x_s, xl_r.at[i], right).start()
        remote(src, src, x_s, xr_r.at[i], left).start()
        remote(src, src, x_s, mt_r.at[i], other).start()

    def spread_near(i):
        near = tok.at[i, block(xl, c)]
        drain(near, xl_r.at[i])
        half = tok.at[i, block(xl, c), low]
        remote(half, half, x_s, hl_r.at[i], right).start()
        remote(near, near, x_s, mt_r.at[i], other).start()
        near = tok.at[i, block(xr, c)]
        drain(near, xr_r.at[i])
        half = tok.at[i, block(xr, c), high]
        remote(half, half, x_s, hr_r.at[i], left).start()
        remote(near, near, x_s, mt_r.at[i], other).start()

    def spread_far(i):
        half = tok.at[i, block(xd, c), low]
        drain(half, hl_r.at[i])
        remote(half, half, x_s, mt_r.at[i], other).start()
        half = tok.at[i, block(xd, c), high]
        drain(half, hr_r.at[i])
        remote(half, half, x_s, mt_r.at[i], other).start()

    def multiply(i):
        qy = lax.rem(y + ORDER[i], 4)
        cut = pl.ds(pl.multiple_of(qy * CHUNK, CHUNK), CHUNK)
        drain(tok.at[i, pl.ds(0, 128)], mt_r.at[i])
        g = dot(tok[i], wg[:, cut], NT)
        u = dot(tok[i], wu[:, cut], NT)
        if i == 0:
            gacc[...] = g
            uacc[...] = u
        else:
            gacc[...] += g
            uacc[...] += u

    for step in range(4 + 3):
        if step < 4:
            spread_own(step)
        if 0 <= step - 1 < 4:
            spread_near(step - 1)
        if 0 <= step - 2 < 4:
            spread_far(step - 2)
        if step == 0:
            loads[3].wait()
            loads[4].wait()
        if 0 <= step - 3 < 4:
            multiply(step - 3)

    g = gacc[...]
    hid[...] = (g / (1.0 + jnp.exp(-g)) * uacc[...]).astype(BF16)
    loads[5].wait()

    def contribute(i):
        qy = lax.rem(y + ORDER[i], 4)
        cut = pl.ds(pl.multiple_of(qy * CHUNK, CHUNK), CHUNK)
        part[i] = dot(hid[...], wd[:, cut], NN).astype(BF16).reshape(2, 128, CHUNK)
        remote(part.at[i, 1 - c], mate.at[i], y_s, my_r.at[i], other).start()

    def pair_up(i):
        drain(mate.at[i], my_r.at[i])
        both = part[i, c].astype(F32) + mate[i].astype(F32)
        zsum[i] = both.astype(BF16).reshape(4, SLOTS, CHUNK)
        remote(zsum.at[i, xd, :, low], hop_l.at[i], y_s, yl_r.at[i], right).start()
        remote(zsum.at[i, xd, :, high], hop_r.at[i], y_s, yr_r.at[i], left).start()
        remote(zsum.at[i, xr, :, high], fin.at[i, 0], y_s, fin_r.at[i], right).start()
        remote(zsum.at[i, xl, :, low], fin.at[i, 2], y_s, fin_r.at[i], left).start()

    def pass_on(i):
        drain(hop_l.at[i], yl_r.at[i])
        zsum[i, xr, :, low] = (
            zsum[i, xr, :, low].astype(F32) + hop_l[i].astype(F32)
        ).astype(BF16)
        remote(zsum.at[i, xr, :, low], fin.at[i, 1], y_s, fin_r.at[i], right).start()
        drain(hop_r.at[i], yr_r.at[i])
        zsum[i, xl, :, high] = (
            zsum[i, xl, :, high].astype(F32) + hop_r[i].astype(F32)
        ).astype(BF16)
        remote(zsum.at[i, xl, :, high], fin.at[i, 3], y_s, fin_r.at[i], left).start()

    def give_back(i):
        qy = lax.rem(y + ORDER[i], 4)
        drain(fin.at[i], fin_r.at[i])
        for half in range(2):
            lanes = pl.ds(half * HALF, HALF)
            whole = (
                zsum[i, x, :, lanes].astype(F32)
                + fin[i, 1 - half].astype(F32)
                + fin[i, 2 + half].astype(F32)
            ).astype(BF16)
            for k in range(4):
                back[qy * 8 + half * 4 + k] = whole[:, k * HD : (k + 1) * HD]

        def send_back(k, carry):
            peer = qy * 8 + lax.rem(z + k, 8)
            remote(back.at[peer], ret.at[me], bk_s, bk_r, {"expert": peer}).start()
            return carry

        lax.fori_loop(1 if ORDER[i] == 0 else 0, 8, send_back, 0)

    for step in range(4 + 3):
        if step < 4:
            contribute(step)
        if 0 <= step - 1 < 4:
            pair_up(step - 1)
        if 0 <= step - 2 < 4:
            pass_on(step - 2)
        if 0 <= step - 3 < 4:
            give_back(step - 3)
    ret[me] = back[me]

    first_gate = 1.0 / (1.0 + jnp.exp(-gap))
    second_gate = 1.0 / (1.0 + jnp.exp(gap))
    drain(ret.at[0 : PEERS - 1], bk_r)
    arrived = ret[...].reshape(PEERS * SLOTS, HD)
    moe = first_gate * dot(comb0, arrived, NN) + second_gate * dot(comb1, arrived, NN)
    late = iota((ROWS, 1), 0) >= 32
    active = jnp.where(late, 1 - stop_ref[0, 1], 1 - stop_ref[0, 0]).astype(F32)
    updated = residual + active * (attn_proj + moe)
    out_ref[...] = updated.astype(BF16).reshape(STEPS, 1, 32, HD)

    drain(att.at[0 : PEERS - 1], att_s)
    drain(stats.at[0 : PEERS - 1], st_s)
    drain(disp.at[0 : PEERS - 1], dp_s)
    drain(tok.at[:, 0:224], x_s)
    drain(tok.at[:, 0:224], y_s)
    drain(ret.at[0 : PEERS - 1], bk_s)


def on_device(
    queries, cache_keys, cache_values, new_keys, new_values, cache_len, o_proj, residual_in,
    norm_gain, router, expert_gate, expert_up, expert_down, routes, answers, stop_mask,
):
    vmem = pl.BlockSpec(memory_space=pltpu.VMEM)
    smem = pl.BlockSpec(memory_space=pltpu.SMEM)
    anywhere = pl.BlockSpec(memory_space=pl.ANY)
    dma = pltpu.SemaphoreType.DMA
    return pl.pallas_call(
        layer,
        out_shape=(
            jax.ShapeDtypeStruct((STEPS, 1, 32, HD), BF16),
            jax.ShapeDtypeStruct((STEPS, 1, ANSWERS), F32),
        ),
        in_specs=[vmem] * 3 + [smem] + [vmem] * 4 + [smem] * 2 + [anywhere] * 6,
        out_specs=(vmem, vmem),
        scratch_shapes=[
            pltpu.VMEM((512, 512), BF16),
            pltpu.VMEM((512, 512), BF16),
            pltpu.VMEM((2048, HD), BF16),
            pltpu.VMEM((LOCAL, D), BF16),
            pltpu.VMEM((LOCAL, D), BF16),
            pltpu.VMEM((LOCAL, D), BF16),
            pltpu.VMEM((32, HD), F32),
            pltpu.VMEM((2, 32, HD), F32),
            pltpu.VMEM((2, 32, HD), F32),
            pltpu.VMEM((PEERS, 32, HD), BF16),
            pltpu.VMEM((PEERS * 32, HD), F32),
            pltpu.VMEM((ROWS, QH * HD), BF16),
            pltpu.VMEM((PEERS, 4, 128), F32),
            pltpu.VMEM((E, SLOTS, HD), BF16),
            pltpu.VMEM((PEERS, SLOTS, HD), BF16),
            pltpu.VMEM((4, 256, CHUNK), BF16),
            pltpu.VMEM((256, LOCAL), F32),
            pltpu.VMEM((256, LOCAL), F32),
            pltpu.VMEM((256, LOCAL), BF16),
            pltpu.VMEM((4, 2, 128, CHUNK), BF16),
            pltpu.VMEM((4, 128, CHUNK), BF16),
            pltpu.VMEM((4, 4, SLOTS, CHUNK), BF16),
            pltpu.VMEM((4, SLOTS, HALF), BF16),
            pltpu.VMEM((4, SLOTS, HALF), BF16),
            pltpu.VMEM((4, 4, SLOTS, HALF), BF16),
            pltpu.VMEM((PEERS, SLOTS, HD), BF16),
            pltpu.VMEM((PEERS, SLOTS, HD), BF16),
            dma((6,)),
            dma, dma, dma, dma, dma, dma((4,)),
            dma, dma((4,)), dma((4,)), dma((4,)), dma((4,)), dma((4,)),
            dma, dma((4,)), dma((4,)), dma((4,)), dma((4,)), dma, dma,
        ],
        compiler_params=pltpu.CompilerParams(collective_id=0, has_side_effects=True),
        name="decode_layer",
    )(
        queries.reshape(STEPS, QH * HD),
        new_keys.reshape(STEPS, KVH * HD),
        new_values.reshape(STEPS, KVH * HD),
        cache_len,
        residual_in,
        norm_gain,
        router.T,
        routes.transpose(0, 1, 3, 2),
        answers.reshape(1, STEPS),
        stop_mask.reshape(1, STEPS),
        cache_keys.reshape(512, 512),
        cache_values.reshape(512, 512),
        o_proj,
        expert_gate.transpose(0, 2, 1).reshape(LOCAL, D),
        expert_up.transpose(0, 2, 1).reshape(LOCAL, D),
        expert_down.reshape(LOCAL, D),
    )


def solution(mesh):
    placed = (
        P(None, "dp", "expert", None),
        P("dp", "expert", None, None),
        P("dp", "expert", None, None),
        P(None, "dp", "expert", None),
        P(None, "dp", "expert", None),
        P("dp", "expert"),
        P(None, "expert"),
        P(None, "dp", None, "expert"),
        P("expert"),
        P("expert", None),
        P("expert", None, "dp"),
        P("expert", None, "dp"),
        P("expert", "dp", None),
        P(),
        P(None, "dp", "expert"),
        P(None, "dp"),
    )
    return jax.shard_map(
        on_device,
        mesh=mesh,
        in_specs=placed,
        out_specs=(P(None, "dp", None, "expert"), P(None, "dp", None)),
        check_vma=False,
    )
```

```python
import jax
import jax.numpy as jnp
from jax import lax
from jax.experimental import pallas as pl
from jax.experimental.pallas import tpu as pltpu
from jax.sharding import PartitionSpec as P

D = 4096
E = 8
HD = 128
QH = 16
KVH = 4
STEPS = 2
ANSWERS = 128
EPSILON = 1e-05

ROWS = 64
PEERS = 32
LOCAL = 448
CHUNK = 1024
HALF = 512
SLOTS = 32
ORDER = (0, 1, 3, 2)
BACK = (2, 1, 3, 0)
GATHER = (
    "own:0,own:1,near:0,own:2,sown:0,near:1,far:0,own:3,votes:0,near:2,far:1,near:3,snear:0,"
    "far:2,mul:0,far:3,sfar:0,mul:1,mul:2,mul:3"
)
RETURN = (
    "con:0,con:1,pair:0,con:2,pair:1,con:3,pair:2,pass:0,pair:3,pass:1,pass:2,give:0,"
    "pass:3,give:1,give:2,give:3"
)

MESH = pl.DeviceIdType.MESH
F32 = jnp.float32
BF16 = jnp.bfloat16
NT = (((1,), (1,)), ((), ()))
NN = (((1,), (0,)), ((), ()))
NEG = -1e30


def dot(a, b, dims, precision=None):
    return lax.dot_general(a, b, dims, precision=precision, preferred_element_type=F32)


def iota(shape, dim):
    return lax.broadcasted_iota(jnp.int32, shape, dim)


def remote(src, dst, send_sem, recv_sem, device):
    return pltpu.make_async_remote_copy(
        src_ref=src,
        dst_ref=dst,
        send_sem=send_sem,
        recv_sem=recv_sem,
        device_id=device,
        device_id_type=MESH,
    )


def drain(ref, sem):
    pltpu.make_async_copy(ref, ref, sem).wait()


def layer(
    q_hbm, nk_hbm, nv_hbm, len_hbm, res_hbm, gain_hbm, router_hbm, routes_hbm, ans_hbm, stop_hbm,
    kc_ref, vc_ref, wo_hbm, wg_hbm, wu_hbm, wd_hbm,
    out_ref, share_ref,
    q_ref, nk_ref, nv_ref, res_ref, gain_ref, router_ref, routes_ref, ans_ref, stop_ref,
    keys, values, wo, wg, wu, wd,
    qs, nks, nvs, att, attf, attm, stats, votes, packed, tok, invs, gacc, uacc, hid,
    part, mate, zsum, hop_l, hop_r, fin, back, ret,
    load_sem, att_s, att_r, st_s, st_r, vt_s, vt_r, dp_s, dp_r,
    x_s, xl_r, xr_r, hl_r, hr_r, mt_r, y_s, my_r, yl_r, yr_r, fin_r, bk_s, bk_r, in_s, in_r,
):
    dp = lax.axis_index("dp")
    me = lax.axis_index("expert")
    x, c = lax.div(dp, 2), lax.rem(dp, 2)
    y, z = lax.div(me, 8), lax.rem(me, 8)
    xr, xl, xd = lax.rem(x + 1, 4), lax.rem(x + 3, 4), lax.rem(x + 2, 4)
    right, left, other = {"dp": xr * 2 + c}, {"dp": xl * 2 + c}, {"dp": x * 2 + 1 - c}
    expert = lax.div(me, 4)

    def everyone(start):
        for dy in (2, 1, 3, 0):
            yd = lax.rem(y + dy, 4)

            def one(i, carry, dy=dy, yd=yd):
                half = lax.div(i + 1, 2)
                dz = jnp.where(lax.rem(i, 2) == 1, 4 - half, 4 + half)
                start(yd * 8 + lax.rem(z + dz, 8), dy)
                return carry

            lax.fori_loop(0, 7 if dy == 0 else 8, one, 0)

    with jax.named_scope("greet"):
        barrier = pltpu.get_barrier_semaphore()
        everyone(
            lambda peer, dy: pl.semaphore_signal(
                barrier, inc=1, device_id={"expert": peer}, device_id_type=MESH
            )
        )
        for neighbour in (right, left, other):
            pl.semaphore_signal(barrier, inc=1, device_id=neighbour, device_id_type=MESH)

        small = [
            (q_hbm, q_ref),
            (kc_ref, keys),
            (nk_hbm, nk_ref),
            (vc_ref, values),
            (nv_hbm, nv_ref),
            (routes_hbm, routes_ref),
            (ans_hbm, ans_ref),
            (stop_hbm, stop_ref),
            (res_hbm, res_ref),
            (gain_hbm, gain_ref),
            (router_hbm, router_ref),
            (wo_hbm, wo),
            (wg_hbm, wg),
            (wu_hbm, wu),
            (wd_hbm, wd),
        ]
        loads = [
            pltpu.make_async_copy(src, dst, load_sem.at[i]) for i, (src, dst) in enumerate(small)
        ]
        for load in loads:
            load.start()

    with jax.named_scope("attn"):
        for i in (0, 2, 4):
            loads[i].wait()
        qf = q_ref[...].astype(F32)
        nkf = nk_ref[...].astype(F32)
        nvf = nv_ref[...].astype(F32)
        for kv in range(KVH):
            lanes = slice(kv * HD, (kv + 1) * HD)
            for t in range(STEPS):
                for g in range(4):
                    h = kv * 4 + g
                    r = kv * 8 + t * 4 + g
                    qs[r : r + 1, :] = qf[t : t + 1, h * HD : (h + 1) * HD]
            for u in range(STEPS):
                nks[u, kv * 8 : kv * 8 + 8, :] = jnp.broadcast_to(nkf[u : u + 1, lanes], (8, HD))
                nvs[u, kv * 8 : kv * 8 + 8, :] = jnp.broadcast_to(nvf[u : u + 1, lanes], (8, HD))
        scale = HD ** (-0.5)
        qa = qs[...]
        qb = qa.astype(BF16)
        row = iota((32, 1), 0)
        second = lax.rem(lax.div(row, 4), 2) == 1
        fresh0 = jnp.sum(qa * nks[0], axis=1, keepdims=True) * scale
        fresh1 = jnp.sum(qa * nks[1], axis=1, keepdims=True) * scale
        fresh1 = jnp.where(second, fresh1, NEG)
        loads[1].wait()
        scores = jnp.concatenate(
            [
                dot(qb[kv * 8 : kv * 8 + 8], keys[:, kv * HD : (kv + 1) * HD], NT)
                for kv in range(KVH)
            ],
            axis=0,
        )
        scores = scores * scale
        scores = jnp.where(iota((32, 512), 1) < len_hbm[...], scores, NEG)
        top = jnp.maximum(jnp.maximum(jnp.max(scores, axis=1, keepdims=True), fresh0), fresh1)
        old = jnp.exp(scores - top)
        new0 = jnp.exp(fresh0 - top)
        new1 = jnp.exp(fresh1 - top)
        total = jnp.sum(old, axis=1, keepdims=True) + new0 + new1
        old = (old / total).astype(BF16)
        new0 = (new0 / total).astype(BF16).astype(F32)
        new1 = (new1 / total).astype(BF16).astype(F32)
        loads[3].wait()
        mixed_values = jnp.concatenate(
            [
                dot(old[kv * 8 : kv * 8 + 8], values[:, kv * HD : (kv + 1) * HD], NN)
                for kv in range(KVH)
            ],
            axis=0,
        )
        mixed_values = mixed_values + new0 * nvs[0] + new1 * nvs[1]
        att[me] = mixed_values.astype(BF16)

    with jax.named_scope("barrier"):
        pl.semaphore_wait(barrier, PEERS + 2)

    with jax.named_scope("sendatt"):
        everyone(
            lambda peer, dy: remote(
                att.at[me], att.at[me], att_s, att_r, {"expert": peer}
            ).start()
        )

    with jax.named_scope("slots"):
        for i in range(5, 12):
            loads[i].wait()
        picks = jnp.concatenate([routes_ref[0, dp], routes_ref[1, dp]], axis=1)
        pick0, pick1 = picks[0:1, :], picks[1:2, :]
        names = iota((E, ROWS), 0)
        hot0, hot1 = (names == pick0).astype(F32), (names == pick1).astype(F32)
        a, b = iota((ROWS, ROWS), 0), iota((ROWS, ROWS), 1)
        before = ((a < b) & (lax.div(a, 32) == lax.div(b, 32))).astype(F32)
        earlier = dot((hot0 + hot1).astype(BF16), before.astype(BF16), NN)
        step_base = lax.div(iota((1, ROWS), 1), 32) * 16
        place0 = jnp.sum(earlier * hot0, axis=0, keepdims=True).astype(jnp.int32)
        place1 = jnp.sum(earlier * hot1, axis=0, keepdims=True).astype(jnp.int32)
        slot0 = pick0 * SLOTS + step_base + place0
        slot1 = pick1 * SLOTS + step_base + place1
        slots = iota((E * SLOTS, ROWS), 0)
        table = ((slots == slot0) | (slots == slot1)).astype(F32).astype(BF16)
        eye = a == b
        sign = hot0 - hot1
        sign_rows = dot(eye.astype(F32).astype(BF16), sign.astype(BF16), NT)
        moving = 1 - stop_ref[...]
        lanes = iota((1, ANSWERS), 1)
        for t in range(STEPS):
            votes[me, t : t + 1, :] = (lanes == ans_ref[:, t : t + 1]).astype(F32) * moving[
                :, t : t + 1
            ].astype(F32)
        residual = res_ref[...].reshape(ROWS, HD).astype(F32)

    with jax.named_scope("waitatt"):
        drain(att.at[0 : PEERS - 1], att_r)
    with jax.named_scope("oproj"):
        attf[...] = att[...].astype(F32).reshape(PEERS * 32, HD)
        for t in range(STEPS):
            for h in range(QH):
                r = (h // 4) * 8 + t * 4 + h % 4
                attm[t * 32 : (t + 1) * 32, h * HD : (h + 1) * HD] = attf[
                    pl.ds(r, 32, stride=32), :
                ].astype(BF16)
        attn_proj = dot(attm[...], wo[...], NN)
        mixed = residual + attn_proj
        scaled = mixed * gain_ref[...].reshape(1, HD)
        packed[...] = dot(table, scaled.astype(BF16), NN).astype(BF16).reshape(E, SLOTS, HD)

    def block(xp, cp):
        return pl.ds(pl.multiple_of((cp * 4 + xp) * SLOTS, SLOTS), SLOTS)

    with jax.named_scope("sendtok"):
        for dy in ORDER:
            yd = lax.rem(y + dy, 4)

            def send_tokens(i, carry, dy=dy, yd=yd):
                peer = yd * 8 + lax.rem(z + i, 8)
                remote(
                    packed.at[lax.div(peer, 4)],
                    tok.at[ORDER.index((4 - dy) % 4), z, block(x, c)],
                    dp_s,
                    dp_r.at[ORDER.index((4 - dy) % 4)],
                    {"expert": peer},
                ).start()
                return carry

            lax.fori_loop(1 if dy == 0 else 0, 8, send_tokens, 0)
        tok[0, z, block(x, c)] = packed[expert]

    with jax.named_scope("stats"):
        squares = jnp.sum(mixed * mixed, axis=1, keepdims=True)
        logits = dot(scaled, router_ref[...], NT, lax.Precision.HIGHEST)
        apart = jnp.sum(logits * sign_rows, axis=1, keepdims=True)
        lane, line = iota((ROWS, 128), 1), iota((ROWS, 128), 0)
        line_up = jnp.where(lane == line, squares, jnp.where(lane == line + ROWS, apart, 0.0))
        stats[me] = jnp.sum(line_up, axis=0, keepdims=True)
        everyone(
            lambda peer, dy: remote(
                stats.at[me], stats.at[me], st_s, st_r, {"expert": peer}
            ).start()
        )

    with jax.named_scope("comb"):
        col0 = jnp.sum(
            jnp.where(eye, jnp.broadcast_to(slot0, (ROWS, ROWS)), 0), axis=1, keepdims=True
        )
        col1 = jnp.sum(
            jnp.where(eye, jnp.broadcast_to(slot1, (ROWS, ROWS)), 0), axis=1, keepdims=True
        )
        cols = iota((ROWS, PEERS * SLOTS), 1)
        ids = lax.div(cols, 128) * SLOTS + lax.rem(cols, SLOTS)
        comb0 = (ids == col0).astype(F32).astype(BF16)
        comb1 = (ids == col1).astype(F32).astype(BF16)

    low, high = pl.ds(0, HALF), pl.ds(HALF, HALF)
    first, last = pl.ds(0, 4), pl.ds(4, 4)

    def spread_own(i):
        src = tok.at[i, :, block(x, c)]
        drain(tok.at[i, pl.ds(0, 7 if i == 0 else 8), block(x, c)], dp_r.at[i])
        remote(src, src, x_s, xl_r.at[i], right).start()
        remote(src, src, x_s, xr_r.at[i], left).start()
        remote(src, src, x_s, mt_r.at[i], other).start()

    def spread_near(i):
        near = tok.at[i, :, block(xl, c)]
        drain(near, xl_r.at[i])
        half = tok.at[i, first, block(xl, c)]
        remote(half, half, x_s, hl_r.at[i], right).start()
        remote(near, near, x_s, mt_r.at[i], other).start()
        near = tok.at[i, :, block(xr, c)]
        drain(near, xr_r.at[i])
        half = tok.at[i, last, block(xr, c)]
        remote(half, half, x_s, hr_r.at[i], left).start()
        remote(near, near, x_s, mt_r.at[i], other).start()

    def spread_far(i):
        half = tok.at[i, first, block(xd, c)]
        drain(half, hl_r.at[i])
        remote(half, half, x_s, mt_r.at[i], other).start()
        half = tok.at[i, last, block(xd, c)]
        drain(half, hr_r.at[i])
        remote(half, half, x_s, mt_r.at[i], other).start()

    def multiply(i):
        qy = lax.rem(y + ORDER[i], 4)
        cut = pl.ds(pl.multiple_of(qy * CHUNK, CHUNK), CHUNK)
        drain(tok.at[i, :, pl.ds(0, 128)], mt_r.at[i])
        if i == 0:
            loads[12].wait()
            loads[13].wait()
        here = jnp.concatenate([tok[i, k] for k in range(8)], axis=1)
        g = dot(here, wg[:, cut], NT)
        u = dot(here, wu[:, cut], NT)
        if i == 0:
            gacc[...] = g
            uacc[...] = u
        else:
            gacc[...] += g
            uacc[...] += u

    def slot_of(xp, cp):
        return cp * 4 + xp

    def scales_own(i):
        drain(stats.at[0 : PEERS - 1], st_r)
        sums = jnp.sum(stats[...], axis=0)
        inv_row = lax.rsqrt(sums[:, 0:ROWS] * (1.0 / D) + EPSILON)
        gap_row = sums[:, ROWS:128] * inv_row
        mine = iota((SLOTS, ROWS), 0) + expert * SLOTS
        own_table = ((mine == slot0) | (mine == slot1)).astype(F32)
        own_inv = jnp.sum(own_table * inv_row, axis=1, keepdims=True)
        own_row = jnp.sum(
            jnp.where(iota((SLOTS, 128), 0) == iota((SLOTS, 128), 1), own_inv, 0.0),
            axis=0,
            keepdims=True,
        )
        invs[slot_of(x, c)] = own_row
        src = invs.at[slot_of(x, c)]
        remote(src, src, in_s, in_r.at[0], right).start()
        remote(src, src, in_s, in_r.at[1], left).start()
        remote(src, src, in_s, in_r.at[3], other).start()
        return jnp.sum(
            jnp.where(eye, jnp.broadcast_to(gap_row, (ROWS, ROWS)), 0.0), axis=1, keepdims=True
        )

    def scales_near(i):
        src = invs.at[slot_of(xl, c)]
        drain(src, in_r.at[0])
        remote(src, src, in_s, in_r.at[2], right).start()
        remote(src, src, in_s, in_r.at[3], other).start()
        src = invs.at[slot_of(xr, c)]
        drain(src, in_r.at[1])
        remote(src, src, in_s, in_r.at[3], other).start()

    def scales_far(i):
        src = invs.at[slot_of(xd, c)]
        drain(src, in_r.at[2])
        remote(src, src, in_s, in_r.at[3], other).start()

    def send_votes(i):
        everyone(
            lambda peer, dy: remote(
                votes.at[me], votes.at[me], vt_s, vt_r, {"expert": peer}
            ).start()
        )

    def contribute(i):
        qy = lax.rem(y + BACK[i], 4)
        cut = pl.ds(pl.multiple_of(qy * CHUNK, CHUNK), CHUNK)
        part[i] = dot(hid[...], wd[:, cut], NN).astype(BF16).reshape(2, 128, CHUNK)
        remote(part.at[i, 1 - c], mate.at[i], y_s, my_r.at[i], other).start()

    def pair_up(i):
        drain(mate.at[i], my_r.at[i])
        both = part[i, c].astype(F32) + mate[i].astype(F32)
        zsum[i] = both.astype(BF16).reshape(4, SLOTS, CHUNK)
        remote(zsum.at[i, xd, :, low], hop_l.at[i], y_s, yl_r.at[i], right).start()
        remote(zsum.at[i, xd, :, high], hop_r.at[i], y_s, yr_r.at[i], left).start()
        remote(zsum.at[i, xr, :, high], fin.at[i, 0], y_s, fin_r.at[i], right).start()
        remote(zsum.at[i, xl, :, low], fin.at[i, 2], y_s, fin_r.at[i], left).start()

    def pass_on(i):
        drain(hop_l.at[i], yl_r.at[i])
        zsum[i, xr, :, low] = (
            zsum[i, xr, :, low].astype(F32) + hop_l[i].astype(F32)
        ).astype(BF16)
        remote(zsum.at[i, xr, :, low], fin.at[i, 1], y_s, fin_r.at[i], right).start()
        drain(hop_r.at[i], yr_r.at[i])
        zsum[i, xl, :, high] = (
            zsum[i, xl, :, high].astype(F32) + hop_r[i].astype(F32)
        ).astype(BF16)
        remote(zsum.at[i, xl, :, high], fin.at[i, 3], y_s, fin_r.at[i], left).start()

    def give_back(i):
        qy = lax.rem(y + BACK[i], 4)
        drain(fin.at[i], fin_r.at[i])
        for half in range(2):
            lanes = pl.ds(half * HALF, HALF)
            whole = (
                zsum[i, x, :, lanes].astype(F32)
                + fin[i, 1 - half].astype(F32)
                + fin[i, 2 + half].astype(F32)
            ).astype(BF16)
            for k in range(4):
                back[qy * 8 + half * 4 + k] = whole[:, k * HD : (k + 1) * HD]

        def send_back(k, carry):
            half = lax.div(k + 1, 2)
            dz = jnp.where(lax.rem(k, 2) == 1, 4 - half, 4 + half)
            peer = qy * 8 + lax.rem(z + dz, 8)
            remote(back.at[peer], ret.at[me], bk_s, bk_r, {"expert": peer}).start()
            return carry

        lax.fori_loop(0, 7 if BACK[i] == 0 else 8, send_back, 0)

    named = {
        "own": spread_own, "near": spread_near, "far": spread_far, "mul": multiply,
        "sown": scales_own, "snear": scales_near, "sfar": scales_far, "votes": send_votes,
        "con": contribute, "pair": pair_up, "pass": pass_on, "give": give_back,
    }

    def run(plan):
        given = {}
        for word in plan.split(","):
            name, i = word.split(":")
            with jax.named_scope(name + i):
                given[name] = named[name](int(i))
        return given

    given = run(GATHER)
    gap = given["sown"]

    with jax.named_scope("hid"):
        drain(invs.at[0:4], in_r.at[3])
        column = jnp.concatenate(
            [
                jnp.sum(
                    jnp.where(iota((SLOTS, 128), 0) == iota((SLOTS, 128), 1), invs[n], 0.0),
                    axis=1,
                    keepdims=True,
                )
                for n in range(8)
            ],
            axis=0,
        )
        g = gacc[...] * column
        hid[...] = (g / (1.0 + jnp.exp(-g)) * (uacc[...] * column)).astype(BF16)
        loads[14].wait()

    run(RETURN)
    with jax.named_scope("gate"):
        ret[me] = back[me]
        first_gate = 1.0 / (1.0 + jnp.exp(-gap))
        second_gate = 1.0 / (1.0 + jnp.exp(gap))
        drain(votes.at[0 : PEERS - 1], vt_r)
        sums = jnp.sum(votes[...], axis=0)
        tally0 = sums[0:1, :]
        tally1 = tally0 + sums[1:2, :]
        share_ref[0] = tally0 / jnp.maximum(jnp.sum(tally0, axis=1, keepdims=True), 1.0)
        share_ref[1] = tally1 / jnp.maximum(jnp.sum(tally1, axis=1, keepdims=True), 1.0)
        late = iota((ROWS, 1), 0) >= 32
        active = jnp.where(late, moving[:, 1:2], moving[:, 0:1]).astype(F32)
    with jax.named_scope("waitret"):
        drain(ret.at[0 : PEERS - 1], bk_r)
    with jax.named_scope("final"):
        arrived = ret[...].reshape(PEERS * SLOTS, HD)
        moe = first_gate * dot(comb0, arrived, NN) + second_gate * dot(comb1, arrived, NN)
        updated = residual + active * (attn_proj + moe)
        out_ref[...] = updated.astype(BF16).reshape(STEPS, 1, 32, HD)

    with jax.named_scope("drain"):
        drain(att.at[0 : PEERS - 1], att_s)
        drain(stats.at[0 : PEERS - 1], st_s)
        drain(votes.at[0 : PEERS - 1], vt_s)
        drain(ret.at[0 : PEERS - 1], dp_s)
        drain(tok.at[:, :, 0:224], x_s)
        drain(tok.at[:, :, 0:224], y_s)
        drain(ret.at[0 : PEERS - 1], bk_s)
        drain(invs.at[0:7], in_s)


def on_device(
    queries, cache_keys, cache_values, new_keys, new_values, cache_len, o_proj, residual_in,
    norm_gain, router, expert_gate, expert_up, expert_down, routes, answers, stop_mask,
):
    vmem = pl.BlockSpec(memory_space=pltpu.VMEM)
    anywhere = pl.BlockSpec(memory_space=pltpu.HBM)
    dma = pltpu.SemaphoreType.DMA
    return pl.pallas_call(
        layer,
        out_shape=(
            pltpu.VMEM((STEPS, 1, 32, HD), BF16),
            pltpu.VMEM((STEPS, 1, ANSWERS), F32),
        ),
        in_specs=[anywhere] * 3 + [vmem] + [anywhere] * 12,
        out_specs=(vmem, vmem),
        scratch_shapes=[
            pltpu.VMEM((STEPS, QH * HD), BF16),
            pltpu.VMEM((STEPS, KVH * HD), BF16),
            pltpu.VMEM((STEPS, KVH * HD), BF16),
            pltpu.VMEM((STEPS, 1, 32, HD), BF16),
            pltpu.VMEM((HD,), F32),
            pltpu.VMEM((E, HD), F32),
            pltpu.VMEM((STEPS, 8, 2, 32), jnp.int32),
            pltpu.VMEM((1, STEPS), jnp.int32),
            pltpu.VMEM((1, STEPS), jnp.int32),
            pltpu.VMEM((512, 512), BF16),
            pltpu.VMEM((512, 512), BF16),
            pltpu.VMEM((2048, HD), BF16),
            pltpu.VMEM((LOCAL, D), BF16),
            pltpu.VMEM((LOCAL, D), BF16),
            pltpu.VMEM((LOCAL, D), BF16),
            pltpu.VMEM((32, HD), F32),
            pltpu.VMEM((2, 32, HD), F32),
            pltpu.VMEM((2, 32, HD), F32),
            pltpu.VMEM((PEERS, 32, HD), BF16),
            pltpu.VMEM((PEERS * 32, HD), F32),
            pltpu.VMEM((ROWS, QH * HD), BF16),
            pltpu.VMEM((PEERS, 1, 128), F32),
            pltpu.VMEM((PEERS, 2, 128), F32),
            pltpu.VMEM((E, SLOTS, HD), BF16),
            pltpu.VMEM((4, 8, 256, HD), BF16),
            pltpu.VMEM((8, 1, 128), F32),
            pltpu.VMEM((256, LOCAL), F32),
            pltpu.VMEM((256, LOCAL), F32),
            pltpu.VMEM((256, LOCAL), BF16),
            pltpu.VMEM((4, 2, 128, CHUNK), BF16),
            pltpu.VMEM((4, 128, CHUNK), BF16),
            pltpu.VMEM((4, 4, SLOTS, CHUNK), BF16),
            pltpu.VMEM((4, SLOTS, HALF), BF16),
            pltpu.VMEM((4, SLOTS, HALF), BF16),
            pltpu.VMEM((4, 4, SLOTS, HALF), BF16),
            pltpu.VMEM((PEERS, SLOTS, HD), BF16),
            pltpu.VMEM((PEERS, SLOTS, HD), BF16),
            dma((15,)),
            dma, dma, dma, dma, dma, dma, dma, dma((4,)),
            dma, dma((4,)), dma((4,)), dma((4,)), dma((4,)), dma((4,)),
            dma, dma((4,)), dma((4,)), dma((4,)), dma((4,)), dma, dma, dma, dma((4,)),
        ],
        compiler_params=pltpu.CompilerParams(collective_id=0, has_side_effects=True),
        name="decode_layer",
    )(
        queries.reshape(STEPS, QH * HD),
        new_keys.reshape(STEPS, KVH * HD),
        new_values.reshape(STEPS, KVH * HD),
        cache_len,
        residual_in,
        norm_gain,
        router.T,
        routes.transpose(0, 1, 3, 2),
        answers.reshape(1, STEPS),
        stop_mask.reshape(1, STEPS),
        cache_keys.reshape(512, 512),
        cache_values.reshape(512, 512),
        o_proj,
        expert_gate.transpose(0, 2, 1).reshape(LOCAL, D),
        expert_up.transpose(0, 2, 1).reshape(LOCAL, D),
        expert_down.reshape(LOCAL, D),
    )


def solution(mesh):
    placed = (
        P(None, "dp", "expert", None),
        P("dp", "expert", None, None),
        P("dp", "expert", None, None),
        P(None, "dp", "expert", None),
        P(None, "dp", "expert", None),
        P("dp", "expert"),
        P(None, "expert"),
        P(None, "dp", None, "expert"),
        P("expert"),
        P("expert", None),
        P("expert", None, "dp"),
        P("expert", None, "dp"),
        P("expert", "dp", None),
        P(),
        P(None, "dp", "expert"),
        P(None, "dp"),
    )
    return jax.shard_map(
        on_device,
        mesh=mesh,
        in_specs=placed,
        out_specs=(P(None, "dp", None, "expert"), P(None, "dp", None)),
        check_vma=False,
    )
```

```python
import jax
import jax.numpy as jnp
from jax import lax
from jax.experimental import pallas as pl
from jax.experimental.pallas import tpu as pltpu
from jax.sharding import PartitionSpec as P

D = 4096
E = 8
HD = 128
QH = 16
KVH = 4
STEPS = 2
ANSWERS = 128
EPSILON = 1e-05

ROWS = 64
PEERS = 32
LOCAL = 448
CHUNK = 1024
HALF = 512
SLOTS = 32
NEAREST = tuple(
    sorted(
        ((dy, dz) for dy in range(4) for dz in range(8)),
        key=lambda o: (min(o[0], 4 - o[0]) + min(o[1], 8 - o[1]), o),
    )
)
FARTHEST = NEAREST[::-1]
GATHER = (
    "own:0,own:1,own:2,near:0,own:3,near:1,sown:0,"
    "near:2,far:0,near:3,far:1,snear:0,votes:0,far:2,"
    "mul:0,far:3,sfar:0,mul:1,mul:2,column:0,mul:3"
)
RETURN = (
    "con:0,con:1,pair:0,con:2,pair:1,con:3,"
    "pass:0,pair:2,pass:1,pair:3,pass:2,give:0,"
    "pass:3,give:1,give:2,give:3"
)

MESH = pl.DeviceIdType.MESH
F32 = jnp.float32
BF16 = jnp.bfloat16
NT = (((1,), (1,)), ((), ()))
NN = (((1,), (0,)), ((), ()))
NEG = -1e30


def dot(a, b, dims, precision=None):
    return lax.dot_general(a, b, dims, precision=precision, preferred_element_type=F32)


def iota(shape, dim):
    return lax.broadcasted_iota(jnp.int32, shape, dim)


def remote(src, dst, send_sem, recv_sem, device):
    return pltpu.make_async_remote_copy(
        src_ref=src,
        dst_ref=dst,
        send_sem=send_sem,
        recv_sem=recv_sem,
        device_id=device,
        device_id_type=MESH,
    )


def drain(ref, sem):
    pltpu.make_async_copy(ref, ref, sem).wait()


def layer(
    q_hbm, nk_hbm, nv_hbm, len_hbm, res_hbm, gain_hbm, router_hbm, routes_hbm, ans_hbm, stop_hbm,
    kc_ref, vc_ref, wo_hbm, wg_hbm, wu_hbm, wd_hbm,
    out_ref, share_ref,
    q_ref, nk_ref, nv_ref, res_ref, gain_ref, router_ref, routes_ref, ans_ref, stop_ref,
    keys, values, wo, wg, wu, wd,
    qs, nks, nvs, att, attf, attm, stats, votes, packed, tok, invs, gacc, uacc, hid,
    part, mate, zsum, hop_l, hop_r, fin, back, ret,
    load_sem, att_s, att_r, st_s, st_r, vt_s, vt_r, dp_s, dp_r,
    x_s, xl_r, xr_r, hl_r, hr_r, mt_r, y_s, my_r, yl_r, yr_r, fin_r, bk_s, bk_r, in_s, in_r,
):
    dp = lax.axis_index("dp")
    me = lax.axis_index("expert")
    x, c = lax.div(dp, 2), lax.rem(dp, 2)
    y, z = lax.div(me, 8), lax.rem(me, 8)
    xr, xl, xd = lax.rem(x + 1, 4), lax.rem(x + 3, 4), lax.rem(x + 2, 4)
    right, left, other = {"dp": xr * 2 + c}, {"dp": xl * 2 + c}, {"dp": x * 2 + 1 - c}
    expert = lax.div(me, 4)

    def at(dy, dz):
        return lax.rem(y + dy, 4) * 8 + lax.rem(z + dz, 8)

    def columns(ref, offsets):
        return jnp.concatenate(
            [ref[:, pl.ds(pl.multiple_of(at(*o) * HD, HD), HD)] for o in offsets], axis=1
        )

    def everyone(start):
        for o in FARTHEST[:-1]:
            start(at(*o))

    with jax.named_scope("greet"):
        small = [
            (q_hbm, q_ref),
            (kc_ref, keys),
            (nk_hbm, nk_ref),
            (vc_ref, values),
            (nv_hbm, nv_ref),
            (routes_hbm, routes_ref),
            (ans_hbm, ans_ref),
            (stop_hbm, stop_ref),
            (res_hbm, res_ref),
            (gain_hbm, gain_ref),
            (router_hbm, router_ref),
            (wo_hbm, wo),
            (wg_hbm, wg),
            (wu_hbm, wu),
            (wd_hbm, wd),
        ]
        loads = [
            pltpu.make_async_copy(src, dst, load_sem.at[i]) for i, (src, dst) in enumerate(small)
        ]
        for load in loads:
            load.start()
        barrier = pltpu.get_barrier_semaphore()
        everyone(
            lambda peer: pl.semaphore_signal(
                barrier, inc=1, device_id={"expert": peer}, device_id_type=MESH
            )
        )
        for neighbour in (right, left, other):
            pl.semaphore_signal(barrier, inc=1, device_id=neighbour, device_id_type=MESH)

    with jax.named_scope("attn"):
        for i in (0, 2, 4):
            loads[i].wait()
        qf = q_ref[...].astype(F32)
        nkf = nk_ref[...].astype(F32)
        nvf = nv_ref[...].astype(F32)
        for kv in range(KVH):
            lanes = slice(kv * HD, (kv + 1) * HD)
            for t in range(STEPS):
                for g in range(4):
                    h = kv * 4 + g
                    r = kv * 8 + t * 4 + g
                    qs[r : r + 1, :] = qf[t : t + 1, h * HD : (h + 1) * HD]
            for u in range(STEPS):
                nks[u, kv * 8 : kv * 8 + 8, :] = jnp.broadcast_to(nkf[u : u + 1, lanes], (8, HD))
                nvs[u, kv * 8 : kv * 8 + 8, :] = jnp.broadcast_to(nvf[u : u + 1, lanes], (8, HD))
        scale = HD ** (-0.5)
        qa = qs[...]
        qb = qa.astype(BF16)
        row = iota((32, 1), 0)
        second = lax.rem(lax.div(row, 4), 2) == 1
        fresh0 = jnp.sum(qa * nks[0], axis=1, keepdims=True) * scale
        fresh1 = jnp.sum(qa * nks[1], axis=1, keepdims=True) * scale
        fresh1 = jnp.where(second, fresh1, NEG)
        loads[1].wait()
        scores = jnp.concatenate(
            [
                dot(qb[kv * 8 : kv * 8 + 8], keys[:, kv * HD : (kv + 1) * HD], NT)
                for kv in range(KVH)
            ],
            axis=0,
        )
        scores = scores * scale
        scores = jnp.where(iota((32, 512), 1) < len_hbm[...], scores, NEG)
        top = jnp.maximum(jnp.maximum(jnp.max(scores, axis=1, keepdims=True), fresh0), fresh1)
        old = jnp.exp(scores - top)
        new0 = jnp.exp(fresh0 - top)
        new1 = jnp.exp(fresh1 - top)
        total = jnp.sum(old, axis=1, keepdims=True) + new0 + new1
        old = (old / total).astype(BF16)
        new0 = (new0 / total).astype(BF16).astype(F32)
        new1 = (new1 / total).astype(BF16).astype(F32)
        loads[3].wait()
        mixed_values = jnp.concatenate(
            [
                dot(old[kv * 8 : kv * 8 + 8], values[:, kv * HD : (kv + 1) * HD], NN)
                for kv in range(KVH)
            ],
            axis=0,
        )
        mixed_values = mixed_values + new0 * nvs[0] + new1 * nvs[1]
        att[me] = mixed_values.astype(BF16)

    with jax.named_scope("barrier"):
        pl.semaphore_wait(barrier, PEERS + 2)

    with jax.named_scope("sendatt"):
        everyone(
            lambda peer: remote(
                att.at[me], att.at[me], att_s, att_r, {"expert": peer}
            ).start()
        )

    with jax.named_scope("slots"):
        for i in range(5, 12):
            loads[i].wait()
        picks = jnp.concatenate([routes_ref[0, dp], routes_ref[1, dp]], axis=1)
        pick0, pick1 = picks[0:1, :], picks[1:2, :]
        names = iota((E, ROWS), 0)
        hot0, hot1 = (names == pick0).astype(F32), (names == pick1).astype(F32)
        a, b = iota((ROWS, ROWS), 0), iota((ROWS, ROWS), 1)
        before = ((a < b) & (lax.div(a, 32) == lax.div(b, 32))).astype(F32)
        earlier = dot((hot0 + hot1).astype(BF16), before.astype(BF16), NN)
        step_base = lax.div(iota((1, ROWS), 1), 32) * 16
        place0 = jnp.sum(earlier * hot0, axis=0, keepdims=True).astype(jnp.int32)
        place1 = jnp.sum(earlier * hot1, axis=0, keepdims=True).astype(jnp.int32)
        slot0 = pick0 * SLOTS + step_base + place0
        slot1 = pick1 * SLOTS + step_base + place1
        slots = iota((E * SLOTS, ROWS), 0)
        table = ((slots == slot0) | (slots == slot1)).astype(F32).astype(BF16)
        eye = a == b
        sign = hot0 - hot1
        sign_rows = dot(eye.astype(F32).astype(BF16), sign.astype(BF16), NT)
        moving = 1 - stop_ref[...]
        lanes = iota((1, ANSWERS), 1)
        for t in range(STEPS):
            votes[me, t : t + 1, :] = (lanes == ans_ref[:, t : t + 1]).astype(F32) * moving[
                :, t : t + 1
            ].astype(F32)
        residual = res_ref[...].reshape(ROWS, HD).astype(F32)

    with jax.named_scope("waitatt"):
        drain(att.at[0 : PEERS - 1], att_r)
    with jax.named_scope("oproj"):
        attf[...] = att[...].astype(F32).reshape(PEERS * 32, HD)
        for t in range(STEPS):
            for h in range(QH):
                r = (h // 4) * 8 + t * 4 + h % 4
                attm[t * 32 : (t + 1) * 32, h * HD : (h + 1) * HD] = attf[
                    pl.ds(r, 32, stride=32), :
                ].astype(BF16)
        attn_proj = dot(attm[...], wo[...], NN)
        mixed = residual + attn_proj
        scaled = mixed * gain_ref[...].reshape(1, HD)
        packed[...] = dot(table, scaled.astype(BF16), NN).astype(BF16).reshape(E, SLOTS, HD)

    def block(xp, cp):
        return pl.ds(pl.multiple_of((cp * 4 + xp) * SLOTS, SLOTS), SLOTS)

    with jax.named_scope("sendtok"):
        for dy, dz in NEAREST[1:]:
            peer = at(dy, dz)
            n = NEAREST.index(((4 - dy) % 4, (8 - dz) % 8))
            remote(
                packed.at[lax.div(peer, 4)],
                tok.at[n // 8, n % 8, block(x, c)],
                dp_s,
                dp_r.at[n // 8],
                {"expert": peer},
            ).start()
        tok[0, 0, block(x, c)] = packed[expert]

    with jax.named_scope("stats"):
        squares = jnp.sum(mixed * mixed, axis=1, keepdims=True)
        logits = dot(scaled, router_ref[...], NT, lax.Precision.HIGHEST)
        apart = jnp.sum(logits * sign_rows, axis=1, keepdims=True)
        lane, line = iota((ROWS, 128), 1), iota((ROWS, 128), 0)
        line_up = jnp.where(lane == line, squares, jnp.where(lane == line + ROWS, apart, 0.0))
        stats[me] = jnp.sum(line_up, axis=0, keepdims=True)
        everyone(
            lambda peer: remote(
                stats.at[me], stats.at[me], st_s, st_r, {"expert": peer}
            ).start()
        )

    with jax.named_scope("comb"):
        col0 = jnp.sum(
            jnp.where(eye, jnp.broadcast_to(slot0, (ROWS, ROWS)), 0), axis=1, keepdims=True
        )
        col1 = jnp.sum(
            jnp.where(eye, jnp.broadcast_to(slot1, (ROWS, ROWS)), 0), axis=1, keepdims=True
        )
        cols = iota((ROWS, PEERS * SLOTS), 1)
        ids = lax.div(cols, 128) * SLOTS + lax.rem(cols, SLOTS)
        comb0 = (ids == col0).astype(F32).astype(BF16)
        comb1 = (ids == col1).astype(F32).astype(BF16)

    low, high = pl.ds(0, HALF), pl.ds(HALF, HALF)
    first, last = pl.ds(0, 4), pl.ds(4, 4)

    def spread_own(i):
        src = tok.at[i, :, block(x, c)]
        drain(tok.at[i, pl.ds(0, 7 if i == 0 else 8), block(x, c)], dp_r.at[i])
        remote(src, src, x_s, xl_r.at[i], right).start()
        remote(src, src, x_s, xr_r.at[i], left).start()
        remote(src, src, x_s, mt_r.at[i], other).start()

    def spread_near(i):
        near = tok.at[i, :, block(xl, c)]
        drain(near, xl_r.at[i])
        half = tok.at[i, first, block(xl, c)]
        remote(half, half, x_s, hl_r.at[i], right).start()
        remote(near, near, x_s, mt_r.at[i], other).start()
        near = tok.at[i, :, block(xr, c)]
        drain(near, xr_r.at[i])
        half = tok.at[i, last, block(xr, c)]
        remote(half, half, x_s, hr_r.at[i], left).start()
        remote(near, near, x_s, mt_r.at[i], other).start()

    def spread_far(i):
        half = tok.at[i, first, block(xd, c)]
        drain(half, hl_r.at[i])
        remote(half, half, x_s, mt_r.at[i], other).start()
        half = tok.at[i, last, block(xd, c)]
        drain(half, hr_r.at[i])
        remote(half, half, x_s, mt_r.at[i], other).start()

    def multiply(i):
        drain(tok.at[i, :, pl.ds(0, 128)], mt_r.at[i])
        if i == 0:
            loads[12].wait()
            loads[13].wait()
        here = jnp.concatenate([tok[i, k] for k in range(8)], axis=1)
        sources = NEAREST[i * 8 : i * 8 + 8]
        g = dot(here, columns(wg, sources), NT)
        u = dot(here, columns(wu, sources), NT)
        if i == 0:
            gacc[...] = g
            uacc[...] = u
        else:
            gacc[...] += g
            uacc[...] += u

    def slot_of(xp, cp):
        return cp * 4 + xp

    def scales_own(i):
        drain(stats.at[0 : PEERS - 1], st_r)
        sums = jnp.sum(stats[...], axis=0)
        inv_row = lax.rsqrt(sums[:, 0:ROWS] * (1.0 / D) + EPSILON)
        gap_row = sums[:, ROWS:128] * inv_row
        mine = iota((SLOTS, ROWS), 0) + expert * SLOTS
        own_table = ((mine == slot0) | (mine == slot1)).astype(F32)
        own_inv = jnp.sum(own_table * inv_row, axis=1, keepdims=True)
        own_row = jnp.sum(
            jnp.where(iota((SLOTS, 128), 0) == iota((SLOTS, 128), 1), own_inv, 0.0),
            axis=0,
            keepdims=True,
        )
        invs[slot_of(x, c)] = own_row
        src = invs.at[slot_of(x, c)]
        remote(src, src, in_s, in_r.at[0], right).start()
        remote(src, src, in_s, in_r.at[1], left).start()
        remote(src, src, in_s, in_r.at[3], other).start()
        return jnp.sum(
            jnp.where(eye, jnp.broadcast_to(gap_row, (ROWS, ROWS)), 0.0), axis=1, keepdims=True
        )

    def scales_near(i):
        src = invs.at[slot_of(xl, c)]
        drain(src, in_r.at[0])
        remote(src, src, in_s, in_r.at[2], right).start()
        remote(src, src, in_s, in_r.at[3], other).start()
        src = invs.at[slot_of(xr, c)]
        drain(src, in_r.at[1])
        remote(src, src, in_s, in_r.at[3], other).start()

    def scales_far(i):
        src = invs.at[slot_of(xd, c)]
        drain(src, in_r.at[2])
        remote(src, src, in_s, in_r.at[3], other).start()

    def scale_column(i):
        drain(invs.at[0:4], in_r.at[3])
        return jnp.concatenate(
            [
                jnp.sum(
                    jnp.where(iota((SLOTS, 128), 0) == iota((SLOTS, 128), 1), invs[n], 0.0),
                    axis=1,
                    keepdims=True,
                )
                for n in range(8)
            ],
            axis=0,
        )

    def send_votes(i):
        everyone(
            lambda peer: remote(
                votes.at[me], votes.at[me], vt_s, vt_r, {"expert": peer}
            ).start()
        )

    def contribute(i):
        owners = FARTHEST[i * 8 : i * 8 + 8]
        part[i] = dot(hid[...], columns(wd, owners), NN).astype(BF16).reshape(2, 128, CHUNK)
        remote(part.at[i, 1 - c], mate.at[i], y_s, my_r.at[i], other).start()

    def pair_up(i):
        drain(mate.at[i], my_r.at[i])
        both = part[i, c].astype(F32) + mate[i].astype(F32)
        zsum[i] = both.astype(BF16).reshape(4, SLOTS, CHUNK)
        remote(zsum.at[i, xd, :, low], hop_l.at[i], y_s, yl_r.at[i], right).start()
        remote(zsum.at[i, xd, :, high], hop_r.at[i], y_s, yr_r.at[i], left).start()
        remote(zsum.at[i, xr, :, high], fin.at[i, 0], y_s, fin_r.at[i], right).start()
        remote(zsum.at[i, xl, :, low], fin.at[i, 2], y_s, fin_r.at[i], left).start()

    def pass_on(i):
        drain(hop_l.at[i], yl_r.at[i])
        zsum[i, xr, :, low] = (
            zsum[i, xr, :, low].astype(F32) + hop_l[i].astype(F32)
        ).astype(BF16)
        remote(zsum.at[i, xr, :, low], fin.at[i, 1], y_s, fin_r.at[i], right).start()
        drain(hop_r.at[i], yr_r.at[i])
        zsum[i, xl, :, high] = (
            zsum[i, xl, :, high].astype(F32) + hop_r[i].astype(F32)
        ).astype(BF16)
        remote(zsum.at[i, xl, :, high], fin.at[i, 3], y_s, fin_r.at[i], left).start()

    def give_back(i):
        drain(fin.at[i], fin_r.at[i])
        for half in range(2):
            lanes = pl.ds(half * HALF, HALF)
            whole = (
                zsum[i, x, :, lanes].astype(F32)
                + fin[i, 1 - half].astype(F32)
                + fin[i, 2 + half].astype(F32)
            ).astype(BF16)
            for k in range(4):
                n = i * 8 + half * 4 + k
                back[n] = whole[:, k * HD : (k + 1) * HD]
                if n < PEERS - 1:
                    peer = {"expert": at(*FARTHEST[n])}
                    remote(back.at[n], ret.at[me], bk_s, bk_r, peer).start()

    named = {
        "own": spread_own, "near": spread_near, "far": spread_far, "mul": multiply,
        "sown": scales_own, "snear": scales_near, "sfar": scales_far, "votes": send_votes, "column": scale_column,
        "con": contribute, "pair": pair_up, "pass": pass_on, "give": give_back,
    }

    def run(plan):
        given = {}
        for word in plan.split(","):
            name, i = word.split(":")
            with jax.named_scope(name + i):
                given[name] = named[name](int(i))
        return given

    given = run(GATHER)
    gap = given["sown"]

    with jax.named_scope("hid"):
        column = given["column"]
        g = gacc[...] * column
        hid[...] = (g / (1.0 + jnp.exp(-g)) * (uacc[...] * column)).astype(BF16)
        loads[14].wait()

    run(RETURN)
    with jax.named_scope("gate"):
        ret[me] = back[PEERS - 1]
        first_gate = 1.0 / (1.0 + jnp.exp(-gap))
        second_gate = 1.0 / (1.0 + jnp.exp(gap))
        drain(votes.at[0 : PEERS - 1], vt_r)
        sums = jnp.sum(votes[...], axis=0)
        tally0 = sums[0:1, :]
        tally1 = tally0 + sums[1:2, :]
        share_ref[0] = tally0 / jnp.maximum(jnp.sum(tally0, axis=1, keepdims=True), 1.0)
        share_ref[1] = tally1 / jnp.maximum(jnp.sum(tally1, axis=1, keepdims=True), 1.0)
        late = iota((ROWS, 1), 0) >= 32
        active = jnp.where(late, moving[:, 1:2], moving[:, 0:1]).astype(F32)
    with jax.named_scope("waitret"):
        drain(ret.at[0 : PEERS - 1], bk_r)
    with jax.named_scope("final"):
        arrived = ret[...].reshape(PEERS * SLOTS, HD)
        moe = first_gate * dot(comb0, arrived, NN) + second_gate * dot(comb1, arrived, NN)
        updated = residual + active * (attn_proj + moe)
        out_ref[...] = updated.astype(BF16).reshape(STEPS, 1, 32, HD)

    with jax.named_scope("drain"):
        drain(att.at[0 : PEERS - 1], att_s)
        drain(stats.at[0 : PEERS - 1], st_s)
        drain(votes.at[0 : PEERS - 1], vt_s)
        drain(ret.at[0 : PEERS - 1], dp_s)
        drain(tok.at[:, :, 0:224], x_s)
        drain(tok.at[:, :, 0:224], y_s)
        drain(ret.at[0 : PEERS - 1], bk_s)
        drain(invs.at[0:7], in_s)


def on_device(
    queries, cache_keys, cache_values, new_keys, new_values, cache_len, o_proj, residual_in,
    norm_gain, router, expert_gate, expert_up, expert_down, routes, answers, stop_mask,
):
    vmem = pl.BlockSpec(memory_space=pltpu.VMEM)
    anywhere = pl.BlockSpec(memory_space=pltpu.HBM)
    dma = pltpu.SemaphoreType.DMA
    return pl.pallas_call(
        layer,
        out_shape=(
            pltpu.VMEM((STEPS, 1, 32, HD), BF16),
            pltpu.VMEM((STEPS, 1, ANSWERS), F32),
        ),
        in_specs=[anywhere] * 3 + [vmem] + [anywhere] * 12,
        out_specs=(vmem, vmem),
        scratch_shapes=[
            pltpu.VMEM((STEPS, QH * HD), BF16),
            pltpu.VMEM((STEPS, KVH * HD), BF16),
            pltpu.VMEM((STEPS, KVH * HD), BF16),
            pltpu.VMEM((STEPS, 1, 32, HD), BF16),
            pltpu.VMEM((HD,), F32),
            pltpu.VMEM((E, HD), F32),
            pltpu.VMEM((STEPS, 8, 2, 32), jnp.int32),
            pltpu.VMEM((1, STEPS), jnp.int32),
            pltpu.VMEM((1, STEPS), jnp.int32),
            pltpu.VMEM((512, 512), BF16),
            pltpu.VMEM((512, 512), BF16),
            pltpu.VMEM((2048, HD), BF16),
            pltpu.VMEM((LOCAL, D), BF16),
            pltpu.VMEM((LOCAL, D), BF16),
            pltpu.VMEM((LOCAL, D), BF16),
            pltpu.VMEM((32, HD), F32),
            pltpu.VMEM((2, 32, HD), F32),
            pltpu.VMEM((2, 32, HD), F32),
            pltpu.VMEM((PEERS, 32, HD), BF16),
            pltpu.VMEM((PEERS * 32, HD), F32),
            pltpu.VMEM((ROWS, QH * HD), BF16),
            pltpu.VMEM((PEERS, 1, 128), F32),
            pltpu.VMEM((PEERS, 2, 128), F32),
            pltpu.VMEM((E, SLOTS, HD), BF16),
            pltpu.VMEM((4, 8, 256, HD), BF16),
            pltpu.VMEM((8, 1, 128), F32),
            pltpu.VMEM((256, LOCAL), F32),
            pltpu.VMEM((256, LOCAL), F32),
            pltpu.VMEM((256, LOCAL), BF16),
            pltpu.VMEM((4, 2, 128, CHUNK), BF16),
            pltpu.VMEM((4, 128, CHUNK), BF16),
            pltpu.VMEM((4, 4, SLOTS, CHUNK), BF16),
            pltpu.VMEM((4, SLOTS, HALF), BF16),
            pltpu.VMEM((4, SLOTS, HALF), BF16),
            pltpu.VMEM((4, 4, SLOTS, HALF), BF16),
            pltpu.VMEM((PEERS, SLOTS, HD), BF16),
            pltpu.VMEM((PEERS, SLOTS, HD), BF16),
            dma((15,)),
            dma, dma, dma, dma, dma, dma, dma, dma((4,)),
            dma, dma((4,)), dma((4,)), dma((4,)), dma((4,)), dma((4,)),
            dma, dma((4,)), dma((4,)), dma((4,)), dma((4,)), dma, dma, dma, dma((4,)),
        ],
        compiler_params=pltpu.CompilerParams(collective_id=0, has_side_effects=True),
        name="decode_layer",
    )(
        queries.reshape(STEPS, QH * HD),
        new_keys.reshape(STEPS, KVH * HD),
        new_values.reshape(STEPS, KVH * HD),
        cache_len,
        residual_in,
        norm_gain,
        router.T,
        routes.transpose(0, 1, 3, 2),
        answers.reshape(1, STEPS),
        stop_mask.reshape(1, STEPS),
        cache_keys.reshape(512, 512),
        cache_values.reshape(512, 512),
        o_proj,
        expert_gate.transpose(0, 2, 1).reshape(LOCAL, D),
        expert_up.transpose(0, 2, 1).reshape(LOCAL, D),
        expert_down.reshape(LOCAL, D),
    )


def solution(mesh):
    placed = (
        P(None, "dp", "expert", None),
        P("dp", "expert", None, None),
        P("dp", "expert", None, None),
        P(None, "dp", "expert", None),
        P(None, "dp", "expert", None),
        P("dp", "expert"),
        P(None, "expert"),
        P(None, "dp", None, "expert"),
        P("expert"),
        P("expert", None),
        P("expert", None, "dp"),
        P("expert", None, "dp"),
        P("expert", "dp", None),
        P(),
        P(None, "dp", "expert"),
        P(None, "dp"),
    )
    return jax.shard_map(
        on_device,
        mesh=mesh,
        in_specs=placed,
        out_specs=(P(None, "dp", None, "expert"), P(None, "dp", None)),
        check_vma=False,
    )
```

```python
import jax
import jax.numpy as jnp
from jax import lax
from jax.experimental import pallas as pl
from jax.experimental.pallas import tpu as pltpu
from jax.sharding import PartitionSpec as P

D = 4096
E = 8
HD = 128
QH = 16
KVH = 4
STEPS = 2
ANSWERS = 128
EPSILON = 1e-05

ROWS = 64
PEERS = 32
LOCAL = 448
CHUNK = 1024
HALF = 512
SLOTS = 32
NEAREST = tuple(
    sorted(
        ((dy, dz) for dy in range(4) for dz in range(8)),
        key=lambda o: (min(o[0], 4 - o[0]) + min(o[1], 8 - o[1]), o),
    )
)
FARTHEST = NEAREST[::-1]
OWNERS = tuple(
    sorted(
        range(PEERS),
        key=lambda k: (k % 8 // 4, k % 8 // 4 * k // 8, k % 8 * 10 + (0, 12, 22, 23)[k // 8], k),
    )
)
GATHER = (
    "own:0,own:1,own:2,near:0,own:3,near:1,sown:0"
)
GATHER_0 = (
    "near:2,far:0,mul:0,near:3,far:1,snear:0,mul:1,far:2,"
    "mul:2,far:3,sfar:0"
)
GATHER_1 = (
    "near:2,far:0,near:3,far:1,snear:0,far:2,far:3,sfar:0,"
    "mul:0,mul:1,mul:2"
)
GATHER_END = (
    "column:0,mul:3"
)
RETURN = (
    "con:0,con:1,pair:0,con:2,pair:1,con:3,votes:0,pass:0,"
    "pair:2,pass:1,pair:3,pass:2,give:0,pass:3,give:1,give:2,"
    "give:3"
)

MESH = pl.DeviceIdType.MESH
F32 = jnp.float32
BF16 = jnp.bfloat16
NT = (((1,), (1,)), ((), ()))
NN = (((1,), (0,)), ((), ()))
NEG = -1e30


def dot(a, b, dims, precision=None):
    return lax.dot_general(a, b, dims, precision=precision, preferred_element_type=F32)


def iota(shape, dim):
    return lax.broadcasted_iota(jnp.int32, shape, dim)


def remote(src, dst, send_sem, recv_sem, device):
    return pltpu.make_async_remote_copy(
        src_ref=src,
        dst_ref=dst,
        send_sem=send_sem,
        recv_sem=recv_sem,
        device_id=device,
        device_id_type=MESH,
    )


def drain(ref, sem):
    pltpu.make_async_copy(ref, ref, sem).wait()


def layer(
    q_hbm, nk_hbm, nv_hbm, len_hbm, res_hbm, gain_hbm, router_hbm, routes_hbm, ans_hbm, stop_hbm,
    kc_ref, vc_ref, wo_hbm, wg_hbm, wu_hbm, wd_hbm,
    out_ref, share_ref,
    q_ref, nk_ref, nv_ref, res_ref, gain_ref, router_ref, routes_ref, ans_ref, stop_ref,
    keys, values, wo, wg, wu, wd,
    qs, nks, nvs, att, attf, attm, stats, votes, packed, tok, invs, gacc, uacc, hid,
    part, mate, zsum, hop_l, hop_r, fin, back, ret,
    load_sem, att_s, att_r, st_s, st_r, vt_s, vt_r, dp_s, dp_r,
    x_s, xl_r, xr_r, hl_r, hr_r, mt_r, y_s, my_r, yl_r, yr_r, fin_r, bk_s, bk_r, in_s, in_r,
):
    dp = lax.axis_index("dp")
    me = lax.axis_index("expert")
    x, c = lax.div(dp, 2), lax.rem(dp, 2)
    y, z = lax.div(me, 8), lax.rem(me, 8)
    xr, xl, xd = lax.rem(x + 1, 4), lax.rem(x + 3, 4), lax.rem(x + 2, 4)
    right, left, other = {"dp": xr * 2 + c}, {"dp": xl * 2 + c}, {"dp": x * 2 + 1 - c}
    expert = lax.div(me, 4)

    def at(dy, dz):
        return lax.rem(y + dy, 4) * 8 + lax.rem(z + dz, 8)

    def columns(ref, offsets):
        return jnp.concatenate(
            [ref[:, pl.ds(pl.multiple_of(at(*o) * HD, HD), HD)] for o in offsets], axis=1
        )

    def everyone(start):
        for o in FARTHEST[:-1]:
            start(at(*o))

    with jax.named_scope("greet"):
        small = [
            (q_hbm, q_ref),
            (kc_ref, keys),
            (nk_hbm, nk_ref),
            (vc_ref, values),
            (nv_hbm, nv_ref),
            (routes_hbm, routes_ref),
            (ans_hbm, ans_ref),
            (stop_hbm, stop_ref),
            (res_hbm, res_ref),
            (gain_hbm, gain_ref),
            (router_hbm, router_ref),
            (wo_hbm, wo),
            (wg_hbm, wg),
            (wu_hbm, wu),
            (wd_hbm, wd),
        ]
        loads = [
            pltpu.make_async_copy(src, dst, load_sem.at[i]) for i, (src, dst) in enumerate(small)
        ]
        for load in loads:
            load.start()
        barrier = pltpu.get_barrier_semaphore()
        everyone(
            lambda peer: pl.semaphore_signal(
                barrier, inc=1, device_id={"expert": peer}, device_id_type=MESH
            )
        )
        for neighbour in (right, left, other):
            pl.semaphore_signal(barrier, inc=1, device_id=neighbour, device_id_type=MESH)

    with jax.named_scope("attn"):
        for i in (0, 2, 4):
            loads[i].wait()
        qf = q_ref[...].astype(F32)
        nkf = nk_ref[...].astype(F32)
        nvf = nv_ref[...].astype(F32)
        for kv in range(KVH):
            lanes = slice(kv * HD, (kv + 1) * HD)
            for t in range(STEPS):
                for g in range(4):
                    h = kv * 4 + g
                    r = kv * 8 + t * 4 + g
                    qs[r : r + 1, :] = qf[t : t + 1, h * HD : (h + 1) * HD]
            for u in range(STEPS):
                nks[u, kv * 8 : kv * 8 + 8, :] = jnp.broadcast_to(nkf[u : u + 1, lanes], (8, HD))
                nvs[u, kv * 8 : kv * 8 + 8, :] = jnp.broadcast_to(nvf[u : u + 1, lanes], (8, HD))
        scale = HD ** (-0.5)
        qa = qs[...]
        qb = qa.astype(BF16)
        row = iota((32, 1), 0)
        second = lax.rem(lax.div(row, 4), 2) == 1
        fresh0 = jnp.sum(qa * nks[0], axis=1, keepdims=True) * scale
        fresh1 = jnp.sum(qa * nks[1], axis=1, keepdims=True) * scale
        fresh1 = jnp.where(second, fresh1, NEG)
        loads[1].wait()
        scores = jnp.concatenate(
            [
                dot(qb[kv * 8 : kv * 8 + 8], keys[:, kv * HD : (kv + 1) * HD], NT)
                for kv in range(KVH)
            ],
            axis=0,
        )
        scores = scores * scale
        scores = jnp.where(iota((32, 512), 1) < len_hbm[...], scores, NEG)
        top = jnp.maximum(jnp.maximum(jnp.max(scores, axis=1, keepdims=True), fresh0), fresh1)
        old = jnp.exp(scores - top)
        new0 = jnp.exp(fresh0 - top)
        new1 = jnp.exp(fresh1 - top)
        total = jnp.sum(old, axis=1, keepdims=True) + new0 + new1
        old = (old / total).astype(BF16)
        new0 = (new0 / total).astype(BF16).astype(F32)
        new1 = (new1 / total).astype(BF16).astype(F32)
        loads[3].wait()
        mixed_values = jnp.concatenate(
            [
                dot(old[kv * 8 : kv * 8 + 8], values[:, kv * HD : (kv + 1) * HD], NN)
                for kv in range(KVH)
            ],
            axis=0,
        )
        mixed_values = mixed_values + new0 * nvs[0] + new1 * nvs[1]
        att[me] = mixed_values.astype(BF16)

    with jax.named_scope("barrier"):
        pl.semaphore_wait(barrier, PEERS + 2)

    with jax.named_scope("sendatt"):
        everyone(
            lambda peer: remote(
                att.at[me], att.at[me], att_s, att_r, {"expert": peer}
            ).start()
        )

    with jax.named_scope("slots"):
        for i in range(5, 12):
            loads[i].wait()
        picks = jnp.concatenate([routes_ref[0, dp], routes_ref[1, dp]], axis=1)
        pick0, pick1 = picks[0:1, :], picks[1:2, :]
        names = iota((E, ROWS), 0)
        hot0, hot1 = (names == pick0).astype(F32), (names == pick1).astype(F32)
        a, b = iota((ROWS, ROWS), 0), iota((ROWS, ROWS), 1)
        before = ((a < b) & (lax.div(a, 32) == lax.div(b, 32))).astype(F32)
        earlier = dot((hot0 + hot1).astype(BF16), before.astype(BF16), NN)
        step_base = lax.div(iota((1, ROWS), 1), 32) * 16
        place0 = jnp.sum(earlier * hot0, axis=0, keepdims=True).astype(jnp.int32)
        place1 = jnp.sum(earlier * hot1, axis=0, keepdims=True).astype(jnp.int32)
        slot0 = pick0 * SLOTS + step_base + place0
        slot1 = pick1 * SLOTS + step_base + place1
        slots = iota((E * SLOTS, ROWS), 0)
        table = ((slots == slot0) | (slots == slot1)).astype(F32).astype(BF16)
        eye = a == b
        sign = hot0 - hot1
        sign_rows = dot(eye.astype(F32).astype(BF16), sign.astype(BF16), NT)
        moving = 1 - stop_ref[...]
        lanes = iota((1, ANSWERS), 1)
        for t in range(STEPS):
            votes[me, t : t + 1, :] = (lanes == ans_ref[:, t : t + 1]).astype(F32) * moving[
                :, t : t + 1
            ].astype(F32)
        residual = res_ref[...].reshape(ROWS, HD).astype(F32)

    with jax.named_scope("waitatt"):
        drain(att.at[0 : PEERS - 1], att_r)
    with jax.named_scope("oproj"):
        attf[...] = att[...].astype(F32).reshape(PEERS * 32, HD)
        for t in range(STEPS):
            for h in range(QH):
                r = (h // 4) * 8 + t * 4 + h % 4
                attm[t * 32 : (t + 1) * 32, h * HD : (h + 1) * HD] = attf[
                    pl.ds(r, 32, stride=32), :
                ].astype(BF16)
        attn_proj = dot(attm[...], wo[...], NN)
        mixed = residual + attn_proj
        scaled = mixed * gain_ref[...].reshape(1, HD)
        packed[...] = dot(table, scaled.astype(BF16), NN).astype(BF16).reshape(E, SLOTS, HD)

    def block(xp, cp):
        return pl.ds(pl.multiple_of((cp * 4 + xp) * SLOTS, SLOTS), SLOTS)

    with jax.named_scope("sendtok"):
        for dy, dz in NEAREST[1:]:
            peer = at(dy, dz)
            n = NEAREST.index(((4 - dy) % 4, (8 - dz) % 8))
            remote(
                packed.at[lax.div(peer, 4)],
                tok.at[n // 8, n % 8, block(x, c)],
                dp_s,
                dp_r.at[n // 8],
                {"expert": peer},
            ).start()
        tok[0, 0, block(x, c)] = packed[expert]

    with jax.named_scope("stats"):
        squares = jnp.sum(mixed * mixed, axis=1, keepdims=True)
        logits = dot(scaled, router_ref[...], NT, lax.Precision.HIGHEST)
        apart = jnp.sum(logits * sign_rows, axis=1, keepdims=True)
        lane, line = iota((ROWS, 128), 1), iota((ROWS, 128), 0)
        line_up = jnp.where(lane == line, squares, jnp.where(lane == line + ROWS, apart, 0.0))
        stats[me] = jnp.sum(line_up, axis=0, keepdims=True)
        everyone(
            lambda peer: remote(
                stats.at[me], stats.at[me], st_s, st_r, {"expert": peer}
            ).start()
        )

    with jax.named_scope("comb"):
        col0 = jnp.sum(
            jnp.where(eye, jnp.broadcast_to(slot0, (ROWS, ROWS)), 0), axis=1, keepdims=True
        )
        col1 = jnp.sum(
            jnp.where(eye, jnp.broadcast_to(slot1, (ROWS, ROWS)), 0), axis=1, keepdims=True
        )
        cols = iota((ROWS, PEERS * SLOTS), 1)
        ids = lax.div(cols, 128) * SLOTS + lax.rem(cols, SLOTS)
        comb0 = (ids == col0).astype(F32).astype(BF16)
        comb1 = (ids == col1).astype(F32).astype(BF16)

    low, high = pl.ds(0, HALF), pl.ds(HALF, HALF)
    first, last = pl.ds(0, 4), pl.ds(4, 4)

    def spread_own(i):
        src = tok.at[i, :, block(x, c)]
        drain(tok.at[i, pl.ds(0, 7 if i == 0 else 8), block(x, c)], dp_r.at[i])
        remote(src, src, x_s, xl_r.at[i], right).start()
        remote(src, src, x_s, xr_r.at[i], left).start()
        remote(src, src, x_s, mt_r.at[i], other).start()

    def spread_near(i):
        near = tok.at[i, :, block(xl, c)]
        drain(near, xl_r.at[i])
        half = tok.at[i, first, block(xl, c)]
        remote(half, half, x_s, hl_r.at[i], right).start()
        remote(near, near, x_s, mt_r.at[i], other).start()
        near = tok.at[i, :, block(xr, c)]
        drain(near, xr_r.at[i])
        half = tok.at[i, last, block(xr, c)]
        remote(half, half, x_s, hr_r.at[i], left).start()
        remote(near, near, x_s, mt_r.at[i], other).start()

    def spread_far(i):
        half = tok.at[i, first, block(xd, c)]
        drain(half, hl_r.at[i])
        remote(half, half, x_s, mt_r.at[i], other).start()
        half = tok.at[i, last, block(xd, c)]
        drain(half, hr_r.at[i])
        remote(half, half, x_s, mt_r.at[i], other).start()

    def multiply(i):
        drain(tok.at[i, :, pl.ds(0, 128)], mt_r.at[i])
        if i == 0:
            loads[12].wait()
            loads[13].wait()
        here = jnp.concatenate([tok[i, k] for k in range(8)], axis=1)
        sources = NEAREST[i * 8 : i * 8 + 8]
        g = dot(here, columns(wg, sources), NT)
        u = dot(here, columns(wu, sources), NT)
        if i == 0:
            gacc[...] = g
            uacc[...] = u
        else:
            gacc[...] += g
            uacc[...] += u

    def slot_of(xp, cp):
        return cp * 4 + xp

    def scales_own(i):
        drain(stats.at[0 : PEERS - 1], st_r)
        sums = jnp.sum(stats[...], axis=0)
        inv_row = lax.rsqrt(sums[:, 0:ROWS] * (1.0 / D) + EPSILON)
        gap_row = sums[:, ROWS:128] * inv_row
        mine = iota((SLOTS, ROWS), 0) + expert * SLOTS
        own_table = ((mine == slot0) | (mine == slot1)).astype(F32)
        own_inv = jnp.sum(own_table * inv_row, axis=1, keepdims=True)
        own_row = jnp.sum(
            jnp.where(iota((SLOTS, 128), 0) == iota((SLOTS, 128), 1), own_inv, 0.0),
            axis=0,
            keepdims=True,
        )
        invs[slot_of(x, c)] = own_row
        src = invs.at[slot_of(x, c)]
        remote(src, src, in_s, in_r.at[0], right).start()
        remote(src, src, in_s, in_r.at[1], left).start()
        remote(src, src, in_s, in_r.at[3], other).start()
        return jnp.sum(
            jnp.where(eye, jnp.broadcast_to(gap_row, (ROWS, ROWS)), 0.0), axis=1, keepdims=True
        )

    def scales_near(i):
        src = invs.at[slot_of(xl, c)]
        drain(src, in_r.at[0])
        remote(src, src, in_s, in_r.at[2], right).start()
        remote(src, src, in_s, in_r.at[3], other).start()
        src = invs.at[slot_of(xr, c)]
        drain(src, in_r.at[1])
        remote(src, src, in_s, in_r.at[3], other).start()

    def scales_far(i):
        src = invs.at[slot_of(xd, c)]
        drain(src, in_r.at[2])
        remote(src, src, in_s, in_r.at[3], other).start()

    def scale_column(i):
        drain(invs.at[0:4], in_r.at[3])
        return jnp.concatenate(
            [
                jnp.sum(
                    jnp.where(iota((SLOTS, 128), 0) == iota((SLOTS, 128), 1), invs[n], 0.0),
                    axis=1,
                    keepdims=True,
                )
                for n in range(8)
            ],
            axis=0,
        )

    def send_votes(i):
        everyone(
            lambda peer: remote(
                votes.at[me], votes.at[me], vt_s, vt_r, {"expert": peer}
            ).start()
        )

    def contribute(i):
        owners = OWNERS[i * 8 : i * 8 + 8]
        wanted = jnp.concatenate([wd[:, k * HD : (k + 1) * HD] for k in owners], axis=1)
        part[i] = dot(hid[...], wanted, NN).astype(BF16).reshape(2, 128, CHUNK)
        remote(part.at[i, 1 - c], mate.at[i], y_s, my_r.at[i], other).start()

    def pair_up(i):
        drain(mate.at[i], my_r.at[i])
        both = part[i, c].astype(F32) + mate[i].astype(F32)
        zsum[i] = both.astype(BF16).reshape(4, SLOTS, CHUNK)
        remote(zsum.at[i, xd, :, low], hop_l.at[i], y_s, yl_r.at[i], right).start()
        remote(zsum.at[i, xd, :, high], hop_r.at[i], y_s, yr_r.at[i], left).start()
        remote(zsum.at[i, xr, :, high], fin.at[i, 0], y_s, fin_r.at[i], right).start()
        remote(zsum.at[i, xl, :, low], fin.at[i, 2], y_s, fin_r.at[i], left).start()

    def pass_on(i):
        drain(hop_l.at[i], yl_r.at[i])
        zsum[i, xr, :, low] = (
            zsum[i, xr, :, low].astype(F32) + hop_l[i].astype(F32)
        ).astype(BF16)
        remote(zsum.at[i, xr, :, low], fin.at[i, 1], y_s, fin_r.at[i], right).start()
        drain(hop_r.at[i], yr_r.at[i])
        zsum[i, xl, :, high] = (
            zsum[i, xl, :, high].astype(F32) + hop_r[i].astype(F32)
        ).astype(BF16)
        remote(zsum.at[i, xl, :, high], fin.at[i, 3], y_s, fin_r.at[i], left).start()

    def send_back(n, owner):
        @pl.when(me != owner)
        def _():
            remote(back.at[n], ret.at[me], bk_s, bk_r, {"expert": owner}).start()

        @pl.when(me == owner)
        def _():
            ret[me] = back[n]

    def give_back(i):
        drain(fin.at[i], fin_r.at[i])
        for half in range(2):
            lanes = pl.ds(half * HALF, HALF)
            whole = (
                zsum[i, x, :, lanes].astype(F32)
                + fin[i, 1 - half].astype(F32)
                + fin[i, 2 + half].astype(F32)
            ).astype(BF16)
            for k in range(4):
                n = i * 8 + half * 4 + k
                back[n] = whole[:, k * HD : (k + 1) * HD]
                send_back(n, OWNERS[n])

    named = {
        "own": spread_own, "near": spread_near, "far": spread_far, "mul": multiply,
        "sown": scales_own, "snear": scales_near, "sfar": scales_far, "votes": send_votes, "column": scale_column,
        "con": contribute, "pair": pair_up, "pass": pass_on, "give": give_back,
    }

    def run(plan):
        given = {}
        for word in plan.split(","):
            name, i = word.split(":")
            with jax.named_scope(name + i):
                given[name] = named[name](int(i))
        return given

    gap = run(GATHER)["sown"]

    @pl.when(c == 0)
    def _():
        run(GATHER_0)

    @pl.when(c == 1)
    def _():
        run(GATHER_1)

    given = run(GATHER_END)

    with jax.named_scope("hid"):
        column = given["column"]
        g = gacc[...] * column
        hid[...] = (g / (1.0 + jnp.exp(-g)) * (uacc[...] * column)).astype(BF16)
        loads[14].wait()

    run(RETURN)
    with jax.named_scope("gate"):
        first_gate = 1.0 / (1.0 + jnp.exp(-gap))
        second_gate = 1.0 / (1.0 + jnp.exp(gap))
        drain(votes.at[0 : PEERS - 1], vt_r)
        sums = jnp.sum(votes[...], axis=0)
        tally0 = sums[0:1, :]
        tally1 = tally0 + sums[1:2, :]
        share_ref[0] = tally0 / jnp.maximum(jnp.sum(tally0, axis=1, keepdims=True), 1.0)
        share_ref[1] = tally1 / jnp.maximum(jnp.sum(tally1, axis=1, keepdims=True), 1.0)
        late = iota((ROWS, 1), 0) >= 32
        active = jnp.where(late, moving[:, 1:2], moving[:, 0:1]).astype(F32)
    with jax.named_scope("waitret"):
        drain(ret.at[0 : PEERS - 1], bk_r)
    with jax.named_scope("final"):
        arrived = ret[...].reshape(PEERS * SLOTS, HD)
        moe = first_gate * dot(comb0, arrived, NN) + second_gate * dot(comb1, arrived, NN)
        updated = residual + active * (attn_proj + moe)
        out_ref[...] = updated.astype(BF16).reshape(STEPS, 1, 32, HD)

    with jax.named_scope("drain"):
        drain(att.at[0 : PEERS - 1], att_s)
        drain(stats.at[0 : PEERS - 1], st_s)
        drain(votes.at[0 : PEERS - 1], vt_s)
        drain(ret.at[0 : PEERS - 1], dp_s)
        drain(tok.at[:, :, 0:224], x_s)
        drain(tok.at[:, :, 0:224], y_s)
        drain(ret.at[0 : PEERS - 1], bk_s)
        drain(invs.at[0:7], in_s)


def on_device(
    queries, cache_keys, cache_values, new_keys, new_values, cache_len, o_proj, residual_in,
    norm_gain, router, expert_gate, expert_up, expert_down, routes, answers, stop_mask,
):
    vmem = pl.BlockSpec(memory_space=pltpu.VMEM)
    anywhere = pl.BlockSpec(memory_space=pltpu.HBM)
    dma = pltpu.SemaphoreType.DMA
    return pl.pallas_call(
        layer,
        out_shape=(
            pltpu.VMEM((STEPS, 1, 32, HD), BF16),
            pltpu.VMEM((STEPS, 1, ANSWERS), F32),
        ),
        in_specs=[anywhere] * 3 + [vmem] + [anywhere] * 12,
        out_specs=(vmem, vmem),
        scratch_shapes=[
            pltpu.VMEM((STEPS, QH * HD), BF16),
            pltpu.VMEM((STEPS, KVH * HD), BF16),
            pltpu.VMEM((STEPS, KVH * HD), BF16),
            pltpu.VMEM((STEPS, 1, 32, HD), BF16),
            pltpu.VMEM((HD,), F32),
            pltpu.VMEM((E, HD), F32),
            pltpu.VMEM((STEPS, 8, 2, 32), jnp.int32),
            pltpu.VMEM((1, STEPS), jnp.int32),
            pltpu.VMEM((1, STEPS), jnp.int32),
            pltpu.VMEM((512, 512), BF16),
            pltpu.VMEM((512, 512), BF16),
            pltpu.VMEM((2048, HD), BF16),
            pltpu.VMEM((LOCAL, D), BF16),
            pltpu.VMEM((LOCAL, D), BF16),
            pltpu.VMEM((LOCAL, D), BF16),
            pltpu.VMEM((32, HD), F32),
            pltpu.VMEM((2, 32, HD), F32),
            pltpu.VMEM((2, 32, HD), F32),
            pltpu.VMEM((PEERS, 32, HD), BF16),
            pltpu.VMEM((PEERS * 32, HD), F32),
            pltpu.VMEM((ROWS, QH * HD), BF16),
            pltpu.VMEM((PEERS, 1, 128), F32),
            pltpu.VMEM((PEERS, 2, 128), F32),
            pltpu.VMEM((E, SLOTS, HD), BF16),
            pltpu.VMEM((4, 8, 256, HD), BF16),
            pltpu.VMEM((8, 1, 128), F32),
            pltpu.VMEM((256, LOCAL), F32),
            pltpu.VMEM((256, LOCAL), F32),
            pltpu.VMEM((256, LOCAL), BF16),
            pltpu.VMEM((4, 2, 128, CHUNK), BF16),
            pltpu.VMEM((4, 128, CHUNK), BF16),
            pltpu.VMEM((4, 4, SLOTS, CHUNK), BF16),
            pltpu.VMEM((4, SLOTS, HALF), BF16),
            pltpu.VMEM((4, SLOTS, HALF), BF16),
            pltpu.VMEM((4, 4, SLOTS, HALF), BF16),
            pltpu.VMEM((PEERS, SLOTS, HD), BF16),
            pltpu.VMEM((PEERS, SLOTS, HD), BF16),
            dma((15,)),
            dma, dma, dma, dma, dma, dma, dma, dma((4,)),
            dma, dma((4,)), dma((4,)), dma((4,)), dma((4,)), dma((4,)),
            dma, dma((4,)), dma((4,)), dma((4,)), dma((4,)), dma, dma, dma, dma((4,)),
        ],
        compiler_params=pltpu.CompilerParams(collective_id=0, has_side_effects=True),
        name="decode_layer",
    )(
        queries.reshape(STEPS, QH * HD),
        new_keys.reshape(STEPS, KVH * HD),
        new_values.reshape(STEPS, KVH * HD),
        cache_len,
        residual_in,
        norm_gain,
        router.T,
        routes.transpose(0, 1, 3, 2),
        answers.reshape(1, STEPS),
        stop_mask.reshape(1, STEPS),
        cache_keys.reshape(512, 512),
        cache_values.reshape(512, 512),
        o_proj,
        expert_gate.transpose(0, 2, 1).reshape(LOCAL, D),
        expert_up.transpose(0, 2, 1).reshape(LOCAL, D),
        expert_down.reshape(LOCAL, D),
    )


def solution(mesh):
    placed = (
        P(None, "dp", "expert", None),
        P("dp", "expert", None, None),
        P("dp", "expert", None, None),
        P(None, "dp", "expert", None),
        P(None, "dp", "expert", None),
        P("dp", "expert"),
        P(None, "expert"),
        P(None, "dp", None, "expert"),
        P("expert"),
        P("expert", None),
        P("expert", None, "dp"),
        P("expert", None, "dp"),
        P("expert", "dp", None),
        P(),
        P(None, "dp", "expert"),
        P(None, "dp"),
    )
    return jax.shard_map(
        on_device,
        mesh=mesh,
        in_specs=placed,
        out_specs=(P(None, "dp", None, "expert"), P(None, "dp", None)),
        check_vma=False,
    )
```
